8 devices in a mesh: sys: 1 (over z), aux: 2 (over y), orb: 4 (over x, core).
Axes of the slice: x: 2, y: 2, z: 1, core: 2. Of those that a mesh axis runs over, the one named last changes fastest.
Arguments:
- b_tensor: float32 [768, 256, 256], P(('sys', 'aux'), 'orb')
- c_alpha: float32 [256, 20], P('sys')
- c_beta: float32 [256, 19], P('sys')
Outputs:
- output 1: float32 [256, 256], P(('sys', 'orb'), 'aux')
- output 2: float32 [256, 256], P(('sys', 'orb'), 'aux')
All inputs are finite; a program needn't handle non-finite values.
Results may differ from the reference program's by a relative error of at most 0.001.
Values are sent between devices in bfloat16 or wider.
A program may use at most 1 GiB of HBM per device.

```python
import math
import jax
import jax.numpy as jnp
from jax import lax

N = 256
NAUX = 768
NALPHA = 20
NBETA = 19

TOP_PRECISION = lax.Precision.HIGHEST


def setup_inputs(seed: int = 0, part: int = 0) -> dict:
    pattern_count = 16
    root_key = jax.random.fold_in(jax.random.key(seed), part)
    key_noise, key_amp, key_orb, key_alpha, key_beta = jax.random.split(root_key, 5)
    amp_scale = (math.sqrt(pattern_count) / (NAUX * (NALPHA + NBETA))) ** 0.5
    raw_noise = jax.random.normal(key_noise, (NAUX, N, N), jnp.float32)
    sym_noise = (raw_noise + jnp.swapaxes(raw_noise, 1, 2)) * (0.5 * amp_scale / math.sqrt(2.0))
    amp_vals = jax.random.normal(key_amp, (NAUX,), jnp.float32) * amp_scale
    orb_pattern = jax.random.normal(key_orb, (pattern_count, N), jnp.float32)
    pattern_rows = jnp.repeat(orb_pattern, NAUX // pattern_count, axis=0)
    outer_prod = pattern_rows[:, :, None] * pattern_rows[:, None, :]
    b_tensor = sym_noise + amp_vals[:, None, None] * outer_prod
    c_alpha = jax.random.normal(key_alpha, (N, NALPHA), jnp.float32) / math.sqrt(N)
    c_beta = jax.random.normal(key_beta, (N, NBETA), jnp.float32) / math.sqrt(N)
    return {'b_tensor': b_tensor, 'c_alpha': c_alpha, 'c_beta': c_beta}


def reference(b_tensor, c_alpha, c_beta):
    b_full = b_tensor.astype(jnp.float32)
    alpha_full = c_alpha.astype(jnp.float32)
    beta_full = c_beta.astype(jnp.float32)
    dens_mat = jnp.dot(alpha_full, alpha_full.T, precision=TOP_PRECISION, preferred_element_type=jnp.float32) + jnp.dot(beta_full, beta_full.T, precision=TOP_PRECISION, preferred_element_type=jnp.float32)
    gamma_vec = jnp.einsum('qms,ms->q', b_full, dens_mat, precision=TOP_PRECISION)
    coul_mat = jnp.einsum('qmn,q->mn', b_full, gamma_vec, precision=TOP_PRECISION)

    def exchange(c_spin):
        half_tr = jnp.einsum('qml,li->qmi', b_full, c_spin, precision=TOP_PRECISION)
        return jnp.einsum('qmi,qni->mn', half_tr, half_tr, precision=TOP_PRECISION)

    return coul_mat - exchange(alpha_full), coul_mat - exchange(beta_full)
```

```python
import jax
import jax.numpy as jnp
from jax import lax
from jax.experimental import pallas as pl
from jax.experimental.pallas import tpu as pltpu
from jax.sharding import PartitionSpec as P

TOP = lax.Precision.HIGHEST
MESH = pl.DeviceIdType.MESH
F32 = jnp.float32

NQ = 384
ROWS = 64
NB = 256
GRP = 4
QGROUPS = 24
CHUNKS = 4
CGROUPS = QGROUPS // CHUNKS
CROWS = CGROUPS * 40
BCH = CGROUPS * GRP * ROWS
TROWS = QGROUPS * 40
AHEAD = 3


def dot(a, b, dims):
    return lax.dot_general(a, b, (dims, ((), ())), precision=TOP, preferred_element_type=F32)


def kernel(b_hbm, ca_hbm, cb_hbm, ga_ref, gb_ref,
           bv, tb, cav, cbv, ct, crep, sacc, gam, grep, kd, ko, kot, gbuf, jp, jr,
           bsem, csem, rs_s, rs_r, ps_s, ps_r, gm_s, gm_r, gk_s, gk_r, j_s, j_r):
    o = lax.axis_index('orb')
    y = lax.axis_index('aux')
    x = o // 2
    c = o % 2
    par = 2 * x + (1 - c)
    far = 2 * (1 - x)

    quarter = (far + c, far + (1 - c), par, o)
    slot = (4 + c, 6, 7, c)

    def bcopy(kind, j):
        start = pl.multiple_of((quarter[kind] * CHUNKS + j) * BCH, BCH)
        return pltpu.make_async_copy(b_hbm.at[pl.ds(start, BCH)], bv.at[pl.ds(start, BCH)], bsem.at[kind, j])

    order = [(k, j) for j in range(CHUNKS) for k in (0, 1)] + [(k, j) for k in (2, 3) for j in range(CHUNKS)]
    ca_copy = pltpu.make_async_copy(ca_hbm, cav, csem.at[0])
    cb_copy = pltpu.make_async_copy(cb_hbm, cbv, csem.at[1])
    ca_copy.start()
    cb_copy.start()
    for k, j in order[:AHEAD]:
        bcopy(k, j).start()

    barrier = pltpu.get_barrier_semaphore()
    for d in range(1, 8):
        other = lax.rem(y * 4 + o + d, 8)
        pl.semaphore_signal(barrier, inc=1, device_id={'aux': other // 4, 'orb': other % 4}, device_id_type=MESH)

    ca_copy.wait()
    cb_copy.wait()

    def assemble(dst, a, b):
        at = a.T
        bt = b.T
        dst[0:16, :] = at[0:16]
        dst[16:32, :] = bt[0:16]
        dst[32:36, :] = at[16:20]
        dst[36:39, :] = bt[16:19]
        dst[39:40, :] = jnp.zeros((1, NB), F32)

    assemble(ct, cav[...], cbv[...])
    my_rows = pl.ds(pl.multiple_of(o * ROWS, ROWS), ROWS)
    own_a = cav[my_rows, :]
    own_b = cbv[my_rows, :]
    assemble(crep, jnp.concatenate([own_a] * GRP, axis=0), jnp.concatenate([own_b] * GRP, axis=0))
    sacc[96:128, :] = jnp.zeros((32, NB), F32)

    low = lax.broadcasted_iota(jnp.int32, (8, 128), 0) < 4

    def half_transform(kind, j):
        bcopy(kind, j).wait()
        first = (quarter[kind] * CHUNKS + j) * CGROUPS

        def body(h, _):
            base = pl.multiple_of((first + 2 * h) * 256, 256)
            r2 = dot(ct[...], bv[pl.ds(base, 512), :], ((1,), (1,)))
            for u in range(2):
                r = r2[:, u * 256:(u + 1) * 256]
                sacc[pl.ds(first + 2 * h + u, 1), :] = jnp.sum(r * crep[...], axis=0, keepdims=True)
                t1 = r[32:40, :128]
                t2 = r[32:40, 128:]
                row = pl.multiple_of(j * CROWS + (2 * h + u) * 40, 8)
                tb[0, slot[kind], pl.ds(row, 16), :] = r[0:16, :128]
                tb[0, slot[kind], pl.ds(row + 16, 16), :] = r[0:16, 128:]
                tb[0, slot[kind], pl.ds(row + 32, 8), :] = jnp.where(low, t1, pltpu.roll(t2, 4, 0))
                tb[1, slot[kind], pl.ds(row, 16), :] = r[16:32, :128]
                tb[1, slot[kind], pl.ds(row + 16, 16), :] = r[16:32, 128:]
                tb[1, slot[kind], pl.ds(row + 32, 8), :] = jnp.where(low, pltpu.roll(t1, 4, 0), t2)
            return 0

        lax.fori_loop(0, CGROUPS // 2, body, 0)

    def part(spin, s, j):
        return tb.at[spin, s, pl.ds(pl.multiple_of(j * CROWS, 8), CROWS)]

    def remote_send(spin, kind, j):
        return pltpu.make_async_remote_copy(
            src_ref=part(spin, slot[kind], j), dst_ref=part(spin, 2 + c, j),
            send_sem=rs_s.at[spin, kind, j], recv_sem=rs_r.at[spin, c, j],
            device_id={'orb': quarter[kind]}, device_id_type=MESH)

    def remote_recv(spin, core, j):
        return pltpu.make_async_remote_copy(
            src_ref=part(spin, 2 + core, j), dst_ref=part(spin, 2 + core, j),
            send_sem=rs_s.at[spin, 0, j], recv_sem=rs_r.at[spin, core, j],
            device_id={'orb': par}, device_id_type=MESH)

    def partner_send(spin, which, j):
        return pltpu.make_async_remote_copy(
            src_ref=part(spin, 6 + which, j), dst_ref=part(spin, (4 + c) if which == 0 else c, j),
            send_sem=ps_s.at[spin, which, j], recv_sem=ps_r.at[spin, which, j],
            device_id={'orb': par}, device_id_type=MESH)

    for n, (k, j) in enumerate(order):
        if n + AHEAD < len(order):
            bcopy(*order[n + AHEAD]).start()
        half_transform(k, j)
        if n == 0:
            pl.semaphore_wait(barrier, 7)
        if k <= 1:
            remote_send(0, k, j).start()
        if k in (1, 2):
            for spin in range(2):
                partner_send(spin, k - 1, j).start()
        if n == 2 * CHUNKS - 1:
            for jj in range(CHUNKS):
                for kk in (0, 1):
                    remote_send(1, kk, jj).start()

    e8 = (lax.broadcasted_iota(jnp.int32, (8, NB), 1) // ROWS == lax.broadcasted_iota(jnp.int32, (8, NB), 0)).astype(F32)
    gam[o] = dot(e8, sacc[...], ((1,), (1,)))

    def gamma_send(d):
        return pltpu.make_async_remote_copy(
            src_ref=gam.at[o], dst_ref=gam.at[o], send_sem=gm_s.at[d], recv_sem=gm_r.at[d],
            device_id={'orb': lax.rem(o + d, 4)}, device_id_type=MESH)

    def gamma_recv(d):
        src = lax.rem(o + 4 - d, 4)
        return pltpu.make_async_remote_copy(
            src_ref=gam.at[src], dst_ref=gam.at[src], send_sem=gm_s.at[d], recv_sem=gm_r.at[d],
            device_id={'orb': par}, device_id_type=MESH)

    for d in range(1, 4):
        gamma_send(d).start()

    left = lax.broadcasted_iota(jnp.int32, (CROWS, 128), 1) < 64

    def merged(spin, s, j):
        a = part(spin, s, j)[...]
        b = part(spin, s + 1, j)[...]
        return jnp.concatenate([jnp.where(left, a, pltpu.roll(b, 64, 1)),
                                jnp.where(left, pltpu.roll(a, 64, 1), b)], axis=0)

    def diag_part(which):
        s = (4, 0)[which]

        def body(j, acc):
            out = []
            for spin in range(2):
                pltpu.make_async_remote_copy(
                    src_ref=part(spin, 6, j), dst_ref=part(spin, (4 + 1 - c) if which == 0 else (1 - c), j),
                    send_sem=ps_s.at[spin, which, j], recv_sem=ps_r.at[spin, which, j],
                    device_id={'orb': par}, device_id_type=MESH).wait_recv()
                m = merged(spin, s, j)
                out.append(acc[spin] + dot(m, m, ((0,), (0,))))
            return tuple(out)
        return body

    zero = jnp.zeros((128, 128), F32)
    acc = lax.fori_loop(0, CHUNKS, diag_part(0), (zero, zero))
    acc = lax.fori_loop(0, CHUNKS, diag_part(1), acc)
    for spin in range(2):
        kd[spin, 0] = acc[spin][:64]
        kd[spin, 1] = acc[spin][64:]

    def block_send(src, spin, cd, xd, yd, base, sidx):
        return pltpu.make_async_remote_copy(
            src_ref=src.at[spin, cd], dst_ref=gbuf.at[spin, base + 2 * y + c],
            send_sem=gk_s.at[spin, sidx, cd], recv_sem=gk_r.at[spin, base + 2 * y + c],
            device_id={'aux': yd, 'orb': 2 * xd + cd}, device_id_type=MESH)

    def each_block(src, spin, xd, yd, base, sidx, act):
        for cd in range(2):
            mine = jnp.logical_and(jnp.logical_and(xd == x, yd == y), c == cd)

            @pl.when(jnp.logical_not(mine))
            def _():
                act(block_send(src, spin, cd, xd, yd, base, sidx))

    start = lambda copy: copy.start()
    wait_send = lambda copy: copy.wait_send()
    for spin in range(2):
        each_block(kd, spin, x, x, 0, 0, start)

    for d in range(1, 4):
        gamma_recv(d).wait_recv()
    gsum = (gam[0] + gam[1]) + (gam[2] + gam[3])
    for k in range(GRP):
        pick = (lax.broadcasted_iota(jnp.int32, (8, 128), 0) == k).astype(F32)
        grep[k] = dot(gsum, pick, ((0,), (0,)))

    def jbody(g, acc):
        for k in range(GRP):
            row = grep[k, pl.ds(g, 1), :]
            base = pl.multiple_of(g * 256 + k * ROWS, ROWS)
            acc = acc + bv[pl.ds(base, ROWS), :] * jnp.concatenate([row, row], axis=1)
        return acc

    jacc = lax.fori_loop(0, NQ // GRP, jbody, jnp.zeros((ROWS, NB), F32))
    jp[0] = jacc[:, :128]
    jp[1] = jacc[:, 128:]
    j_copy = pltpu.make_async_remote_copy(
        src_ref=jp.at[1 - y], dst_ref=jr, send_sem=j_s, recv_sem=j_r,
        device_id={'aux': 1 - y}, device_id_type=MESH)
    j_copy.start()

    for spin in range(2):
        def obody(j, acc):
            for core in range(2):
                remote_recv(spin, core, j).wait_recv()
            return acc + dot(merged(spin, 0, j), merged(spin, 2, j), ((0,), (0,)))
        block = lax.fori_loop(0, CHUNKS, obody, zero)
        ko[spin, 0] = block[:64]
        ko[spin, 1] = block[64:]
        flip = block.T
        kot[spin, 0] = flip[:64]
        kot[spin, 1] = flip[64:]
        each_block(ko, spin, x, 1 - x, 0, 1, start)
        each_block(kot, spin, 1 - x, x, 4, 2, start)

    j_copy.wait()
    jsum = jp[y] + jr[...]

    def block_recv(spin, s):
        return pltpu.make_async_remote_copy(
            src_ref=gbuf.at[spin, s], dst_ref=gbuf.at[spin, s],
            send_sem=gk_s.at[spin, 0, 0], recv_sem=gk_r.at[spin, s],
            device_id={'orb': par}, device_id_type=MESH)

    def finish(src, count):
        for spin, out in ((0, ga_ref), (1, gb_ref)):
            total = src[spin, c]
            for d in range(1, count):
                s = lax.rem(2 * y + c + d, 4) if d < 4 else d
                block_recv(spin, s).wait_recv()
                total = total + gbuf[spin, s]
            out[...] = jsum - total

    @pl.when(x == y)
    def _():
        finish(kd, 4)

    @pl.when(x != y)
    def _():
        finish(ko, 8)

    for spin in range(2):
        each_block(kd, spin, x, x, 0, 0, wait_send)
        each_block(ko, spin, x, 1 - x, 0, 1, wait_send)
        each_block(kot, spin, 1 - x, x, 4, 2, wait_send)
        for j in range(CHUNKS):
            for k in range(2):
                remote_send(spin, k, j).wait_send()
                partner_send(spin, k, j).wait_send()
    for d in range(1, 4):
        gamma_send(d).wait_send()


def solution(mesh):
    def local_build(b_local, c_alpha, c_beta):
        b_rows = b_local.reshape(NQ * ROWS, NB)
        dma = pltpu.SemaphoreType.DMA
        vmem = pltpu.VMEM
        return pl.pallas_call(
            kernel,
            out_shape=[jax.ShapeDtypeStruct((ROWS, 128), F32)] * 2,
            in_specs=[pl.BlockSpec(memory_space=pl.ANY)] * 3,
            out_specs=[pl.BlockSpec(memory_space=vmem)] * 2,
            scratch_shapes=[
                vmem((NQ * ROWS, NB), F32),
                vmem((2, 8, TROWS, 128), F32),
                vmem((NB, 20), F32), vmem((NB, 19), F32),
                vmem((40, NB), F32), vmem((40, NB), F32),
                vmem((128, NB), F32),
                vmem((4, 8, 128), F32),
                vmem((GRP, 128, 128), F32),
                vmem((2, 2, 64, 128), F32), vmem((2, 2, 64, 128), F32), vmem((2, 2, 64, 128), F32),
                vmem((2, 8, 64, 128), F32),
                vmem((2, 64, 128), F32), vmem((64, 128), F32),
                dma((4, CHUNKS)), dma((2,)),
                dma((2, 2, CHUNKS)), dma((2, 2, CHUNKS)),
                dma((2, 2, CHUNKS)), dma((2, 2, CHUNKS)),
                dma((4,)), dma((4,)),
                dma((2, 3, 2)), dma((2, 8)),
                dma, dma,
            ],
            compiler_params=pltpu.CompilerParams(
                collective_id=0, has_side_effects=True, vmem_limit_bytes=56 * 1024 * 1024),
        )(b_rows, c_alpha, c_beta)

    spec_b = P(('sys', 'aux'), 'orb', None)
    spec_c = P('sys', None)
    spec_g = P(('sys', 'orb'), 'aux')
    return jax.shard_map(local_build, mesh=mesh, in_specs=(spec_b, spec_c, spec_c), out_specs=(spec_g, spec_g), check_vma=False)
```

```python
import jax
import jax.numpy as jnp
from jax import lax
from jax.experimental import pallas as pl
from jax.experimental.pallas import tpu as pltpu
from jax.sharding import PartitionSpec as P

TOP = lax.Precision.HIGHEST
MESH = pl.DeviceIdType.MESH
F32 = jnp.float32

NQ = 384
ROWS = 64
NB = 256
GRP = 4
QGROUPS = 24
CHUNKS = 6
CGROUPS = QGROUPS // CHUNKS
CROWS = (CGROUPS * 40, CGROUPS * 38)
BCH = CGROUPS * GRP * ROWS
TROWS = CHUNKS * CROWS[0]
AHEAD = 4
DEPTH = 3


def dot(a, b, dims):
    return lax.dot_general(a, b, (dims, ((), ())), precision=TOP, preferred_element_type=F32)


BF16 = jnp.bfloat16
SHRINK = 1.0 - 2.0 ** -9


def split(v):
    v1 = (v * SHRINK).astype(BF16)
    rest = v - v1.astype(F32)
    v2 = rest.astype(BF16)
    return v1, v2, (rest - v2.astype(F32)).astype(BF16)


def dot16(a, b, dims):
    return lax.dot_general(a, b, (dims, ((), ())), preferred_element_type=F32)


def kernel(b_hbm, ca_hbm, cb_hbm, s_ref, jout_ref,
           bv, tb, cav, cbv, ct, cs, crep, sacc, gam, grep, kd, ko, kot, gbuf, jp, jr,
           bsem, csem, rs_s, rs_r, ps_s, ps_r, gm_s, gm_r, gk_s, gk_r, j_s, j_r):
    o = lax.axis_index('orb')
    y = lax.axis_index('aux')
    x = o // 2
    c = o % 2
    par = 2 * x + (1 - c)
    far = 2 * (1 - x)

    quarter = (far + c, far + (1 - c), par, o)
    slot = (4 + c, 6, 7, c)

    def bcopy(kind, j):
        start = pl.multiple_of((quarter[kind] * CHUNKS + j) * BCH, BCH)
        return pltpu.make_async_copy(b_hbm.at[pl.ds(start, BCH)], bv.at[pl.ds(start, BCH)], bsem.at[kind, j])

    order = [(k, j) for j in range(CHUNKS) for k in (0, 1)] + [(k, j) for k in (2, 3) for j in range(CHUNKS)]
    ca_copy = pltpu.make_async_copy(ca_hbm, cav, csem.at[0])
    cb_copy = pltpu.make_async_copy(cb_hbm, cbv, csem.at[1])
    ca_copy.start()
    cb_copy.start()
    for k, j in order[:AHEAD]:
        bcopy(k, j).start()

    barrier = pltpu.get_barrier_semaphore()
    for d in range(1, 8):
        other = lax.rem(y * 4 + o + d, 8)
        pl.semaphore_signal(barrier, inc=1, device_id={'aux': other // 4, 'orb': other % 4}, device_id_type=MESH)

    ca_copy.wait()
    cb_copy.wait()
    ct[0:16, :] = cav[0:16, :]
    ct[16:32, :] = cbv[0:16, :]
    ct[32:36, :] = cav[16:20, :]
    ct[36:39, :] = cbv[16:19, :]
    ct[39:40, :] = jnp.zeros((1, NB), F32)
    cs[...] = jnp.concatenate([t.astype(F32) for t in split(ct[...])], axis=0).astype(BF16)
    own = ct[:, pl.ds(pl.multiple_of(x * 128, 128), 128)]
    turned = pltpu.roll(own, 64, 1)
    low = lax.broadcasted_iota(jnp.int32, (40, 128), 1) < 64
    own = jnp.where(low, jnp.where(c == 0, own, turned), jnp.where(c == 0, turned, own))
    crep[:, :128] = own
    crep[:, 128:] = own
    sacc[96:128, :] = jnp.zeros((32, NB), F32)

    def part(spin, s, j):
        return tb.at[spin, s, pl.ds(pl.multiple_of(j * CROWS[spin], 8), CROWS[spin])]

    def half_transform(kind, j):
        bcopy(kind, j).wait()
        first = (quarter[kind] * CHUNKS + j) * CGROUPS
        to_a = part(0, slot[kind], j)
        to_b = part(1, slot[kind], j)
        for h in range(CGROUPS // 2):
            base = pl.multiple_of((first + 2 * h) * 256, 256)
            b1, b2, b3 = split(bv[pl.ds(base, 512), :])
            r1 = dot16(cs[...], b1, ((1,), (1,)))
            r2 = dot16(cs[0:80, :], b2, ((1,), (1,)))
            r3 = dot16(cs[0:40, :], b3, ((1,), (1,)))
            r2 = ((r3 + r2[40:80] + r1[80:120]) + (r2[0:40] + r1[40:80])) + r1[0:40]
            for u in range(4):
                p = 4 * h + u
                r = r2[:, u * 128:(u + 1) * 128]
                to_a[16 * p:16 * p + 16, :] = r[0:16]
                to_b[16 * p:16 * p + 16, :] = r[16:32]
                to_a[128 + 4 * p:132 + 4 * p, :] = r[32:36]
                to_b[128 + 3 * p:131 + 3 * p, :] = r[36:39]
            for u in range(2):
                r = r2[:, u * 256:(u + 1) * 256]
                sacc[pl.ds(first + 2 * h + u, 1), :] = jnp.sum(r * crep[...], axis=0, keepdims=True)

    def remote_send(spin, kind, j):
        return pltpu.make_async_remote_copy(
            src_ref=part(spin, slot[kind], j), dst_ref=part(spin, 2 + c, j),
            send_sem=rs_s.at[spin, kind, j], recv_sem=rs_r.at[spin, c, j],
            device_id={'orb': quarter[kind]}, device_id_type=MESH)

    def remote_recv(spin, core, j):
        return pltpu.make_async_remote_copy(
            src_ref=part(spin, 2 + core, j), dst_ref=part(spin, 2 + core, j),
            send_sem=rs_s.at[spin, 0, j], recv_sem=rs_r.at[spin, core, j],
            device_id={'orb': par}, device_id_type=MESH)

    def partner_send(spin, which, j):
        return pltpu.make_async_remote_copy(
            src_ref=part(spin, 6 + which, j), dst_ref=part(spin, (4 + c) if which == 0 else c, j),
            send_sem=ps_s.at[spin, which, j], recv_sem=ps_r.at[spin, which, j],
            device_id={'orb': par}, device_id_type=MESH)

    def partner_recv(spin, which, j):
        return pltpu.make_async_remote_copy(
            src_ref=part(spin, 6, j), dst_ref=part(spin, (5 - c) if which == 0 else (1 - c), j),
            send_sem=ps_s.at[spin, which, j], recv_sem=ps_r.at[spin, which, j],
            device_id={'orb': par}, device_id_type=MESH)

    items = [(spin, k, j) for spin in range(2) for k, j in order[:2 * CHUNKS]]
    issued = [0]

    def issue(upto):
        while issued[0] < min(upto, len(items)):
            n = issued[0]
            if n >= 2 * CHUNKS:
                remote_send(*items[n - DEPTH]).wait_send()
            remote_send(*items[n]).start()
            issued[0] = n + 1

    half_transform(0, 0)
    for k, j in order[AHEAD:]:
        bcopy(k, j).start()
    pl.semaphore_wait(barrier, 7)
    issue(1)
    half_transform(1, 0)
    issue(2)
    issued[0] = 2 * CHUNKS

    def pair(j, _):
        for k in (0, 1):
            half_transform(k, j)
            remote_send(0, k, j).start()
        return 0

    lax.fori_loop(1, CHUNKS, pair, 0)

    def back(j, _):
        for spin in range(2):
            partner_send(spin, 0, j).start()
        half_transform(2, j)
        for spin in range(2):
            partner_send(spin, 1, j).start()
        return 0

    lax.fori_loop(0, CHUNKS, back, 0)

    def home(j, _):
        half_transform(3, j)
        return 0

    lax.fori_loop(0, CHUNKS - 2, home, 0)
    issue(2 * CHUNKS + 1)
    lax.fori_loop(CHUNKS - 2, CHUNKS, home, 0)
    issue(2 * CHUNKS + 2)

    e8 = (lax.broadcasted_iota(jnp.int32, (8, NB), 1) // ROWS == lax.broadcasted_iota(jnp.int32, (8, NB), 0)).astype(F32)
    gam[o] = dot(e8, sacc[...], ((1,), (1,)))

    def gamma_send(d):
        return pltpu.make_async_remote_copy(
            src_ref=gam.at[o], dst_ref=gam.at[o], send_sem=gm_s.at[d], recv_sem=gm_r.at[d],
            device_id={'orb': lax.rem(o + d, 4)}, device_id_type=MESH)

    def gamma_recv(d):
        src = lax.rem(o + 4 - d, 4)
        return pltpu.make_async_remote_copy(
            src_ref=gam.at[src], dst_ref=gam.at[src], send_sem=gm_s.at[d], recv_sem=gm_r.at[d],
            device_id={'orb': par}, device_id_type=MESH)

    for d in range(1, 4):
        gamma_send(d).start()

    def merged(spin, s, j, count=1):
        rows = count * CROWS[spin]
        at = pl.ds(pl.multiple_of(j * CROWS[spin], 8), rows)
        a = tb[spin, s, at]
        b = tb[spin, s + 1, at]
        left = lax.broadcasted_iota(jnp.int32, (rows, 128), 1) < 64
        return jnp.concatenate([jnp.where(left, a, pltpu.roll(b, 64, 1)),
                                jnp.where(left, pltpu.roll(a, 64, 1), b)], axis=0)

    zero = jnp.zeros((128, 128), F32)
    half = CHUNKS // 2
    for spin in range(2):
        acc = zero
        for which in range(2):
            def dbody(h, acc):
                for u in range(half):
                    partner_recv(spin, which, h * half + u).wait_recv()
                m = merged(spin, (4, 0)[which], h * half, half)
                return acc + dot(m, m, ((0,), (0,)))
            acc = lax.fori_loop(0, 2, dbody, acc)
            issue(issued[0] + 1)
        kd[spin, 0] = acc[:64]
        kd[spin, 1] = acc[64:]

    def block_send(src, spin, cd, xd, yd, base, sidx):
        return pltpu.make_async_remote_copy(
            src_ref=src.at[spin, cd], dst_ref=gbuf.at[spin, base + 2 * y + c],
            send_sem=gk_s.at[spin, sidx, cd], recv_sem=gk_r.at[spin, base + 2 * y + c],
            device_id={'aux': yd, 'orb': 2 * xd + cd}, device_id_type=MESH)

    def each_block(src, spin, xd, yd, base, sidx, act):
        for cd in range(2):
            mine = jnp.logical_and(jnp.logical_and(xd == x, yd == y), c == cd)

            @pl.when(jnp.logical_not(mine))
            def _():
                act(block_send(src, spin, cd, xd, yd, base, sidx))

    start = lambda copy: copy.start()
    wait_send = lambda copy: copy.wait_send()
    for spin in range(2):
        each_block(kd, spin, x, x, 0, 0, start)

    for d in range(1, 4):
        gamma_recv(d).wait_recv()
    gsum = (gam[0] + gam[1]) + (gam[2] + gam[3])
    for k in range(GRP):
        pick = (lax.broadcasted_iota(jnp.int32, (8, 128), 0) == k).astype(F32)
        grep[k] = dot(gsum, pick, ((0,), (0,)))

    def jbody(g, acc):
        for k in range(GRP):
            row = grep[k, pl.ds(g, 1), :]
            base = pl.multiple_of(g * 256 + k * ROWS, ROWS)
            acc = acc + bv[pl.ds(base, ROWS), :] * jnp.concatenate([row, row], axis=1)
        return acc

    jacc = lax.fori_loop(0, NQ // GRP, jbody, jnp.zeros((ROWS, NB), F32))
    jp[0] = jacc[:, :128]
    jp[1] = jacc[:, 128:]
    j_copy = pltpu.make_async_remote_copy(
        src_ref=jp.at[1 - y], dst_ref=jr, send_sem=j_s, recv_sem=j_r,
        device_id={'aux': 1 - y}, device_id_type=MESH)
    j_copy.start()
    issue(issued[0] + 1)

    def block_recv(spin, s):
        return pltpu.make_async_remote_copy(
            src_ref=gbuf.at[spin, s], dst_ref=gbuf.at[spin, s],
            send_sem=gk_s.at[spin, 0, 0], recv_sem=gk_r.at[spin, s],
            device_id={'orb': par}, device_id_type=MESH)

    def finish(spin, src, count):
        total = src[spin, c]
        for d in range(1, count):
            s = lax.rem(2 * y + c + d, 4) if d < 4 else d
            block_recv(spin, s).wait_recv()
            total = total + gbuf[spin, s]
        s_ref[spin * 64:spin * 64 + 64, :] = total

    for spin in range(2):
        block = zero
        for j in range(CHUNKS):
            if spin == 1:
                issue(2 * CHUNKS + 2 * j + 1 + DEPTH)
            for core in range(2):
                remote_recv(spin, core, j).wait_recv()
            block = block + dot(merged(spin, 0, j), merged(spin, 2, j), ((0,), (0,)))
        ko[spin, 0] = block[:64]
        ko[spin, 1] = block[64:]
        flip = block.T
        kot[spin, 0] = flip[:64]
        kot[spin, 1] = flip[64:]
        each_block(ko, spin, x, 1 - x, 0, 1, start)
        each_block(kot, spin, 1 - x, x, 4, 2, start)

    j_copy.wait()
    jout_ref[...] = jp[y] + jr[...]

    @pl.when(x == y)
    def _():
        finish(0, kd, 4)
        finish(1, kd, 4)

    @pl.when(x != y)
    def _():
        finish(0, ko, 8)
        finish(1, ko, 8)

    for spin in range(2):
        each_block(kd, spin, x, x, 0, 0, wait_send)
        each_block(ko, spin, x, 1 - x, 0, 1, wait_send)
        each_block(kot, spin, 1 - x, x, 4, 2, wait_send)
        for j in range(CHUNKS):
            for k in range(2):
                partner_send(spin, k, j).wait_send()
    waited = len(items) - DEPTH
    for n, item in enumerate(items):
        if n < 2 * CHUNKS - DEPTH or n >= waited:
            remote_send(*item).wait_send()
    for d in range(1, 4):
        gamma_send(d).wait_send()


def solution(mesh):
    def local_build(b_local, c_alpha, c_beta):
        b_rows = b_local.reshape(NQ * ROWS, NB)
        dma = pltpu.SemaphoreType.DMA
        vmem = pltpu.VMEM
        neg, coul = pl.pallas_call(
            kernel,
            out_shape=[jax.ShapeDtypeStruct((2 * ROWS, 128), F32), jax.ShapeDtypeStruct((ROWS, 128), F32)],
            in_specs=[pl.BlockSpec(memory_space=pl.ANY)] * 3,
            out_specs=[pl.BlockSpec(memory_space=vmem)] * 2,
            scratch_shapes=[
                vmem((NQ * ROWS, NB), F32),
                vmem((2, 8, TROWS, 128), F32),
                vmem((20, NB), F32), vmem((19, NB), F32),
                vmem((40, NB), F32), vmem((120, NB), BF16), vmem((40, NB), F32),
                vmem((128, NB), F32),
                vmem((4, 8, 128), F32),
                vmem((GRP, 128, 128), F32),
                vmem((2, 2, 64, 128), F32), vmem((2, 2, 64, 128), F32), vmem((2, 2, 64, 128), F32),
                vmem((2, 8, 64, 128), F32),
                vmem((2, 64, 128), F32), vmem((64, 128), F32),
                dma((4, CHUNKS)), dma((2,)),
                dma((2, 2, CHUNKS)), dma((2, 2, CHUNKS)),
                dma((2, 2, CHUNKS)), dma((2, 2, CHUNKS)),
                dma((4,)), dma((4,)),
                dma((2, 3, 2)), dma((2, 8)),
                dma, dma,
            ],
            compiler_params=pltpu.CompilerParams(
                collective_id=0, has_side_effects=True, vmem_limit_bytes=56 * 1024 * 1024),
        )(b_rows, c_alpha.T, c_beta.T)
        return coul - neg[:ROWS], coul - neg[ROWS:]

    spec_b = P(('sys', 'aux'), 'orb', None)
    spec_c = P('sys', None)
    spec_g = P(('sys', 'orb'), 'aux')
    return jax.shard_map(local_build, mesh=mesh, in_specs=(spec_b, spec_c, spec_c), out_specs=(spec_g, spec_g), check_vma=False)
```

```python
import jax
import jax.numpy as jnp
from jax import lax
from jax.experimental import pallas as pl
from jax.experimental.pallas import tpu as pltpu
from jax.sharding import PartitionSpec as P

TOP = lax.Precision.HIGHEST
MESH = pl.DeviceIdType.MESH
F32 = jnp.float32

NQ = 384
ROWS = 64
NB = 256
GRP = 4
QGROUPS = 24
CHUNKS = 6
CGROUPS = QGROUPS // CHUNKS
CROWS = (CGROUPS * 40, CGROUPS * 38)
BCH = CGROUPS * GRP * ROWS
TROWS = CHUNKS * CROWS[0]
AHEAD = 4
DEPTH = 3


def dot(a, b, dims):
    return lax.dot_general(a, b, (dims, ((), ())), precision=TOP, preferred_element_type=F32)


BF16 = jnp.bfloat16
SHRINK = 1.0 - 2.0 ** -9


def split(v):
    v1 = (v * SHRINK).astype(BF16)
    rest = v - v1.astype(F32)
    v2 = rest.astype(BF16)
    return v1, v2, (rest - v2.astype(F32)).astype(BF16)


def dot16(a, b, dims):
    return lax.dot_general(a, b, (dims, ((), ())), preferred_element_type=F32)


def kernel(b_hbm, ca_hbm, cb_hbm, s_ref, jout_ref,
           bv, tb, cav, cbv, ct, cs, crep, sacc, gam, grep, kd, ko, kot, gbuf, jp, jr,
           bsem, csem, rs_s, rs_r, ps_s, ps_r, gm_s, gm_r, gk_s, gk_r, j_s, j_r):
    o = lax.axis_index('orb')
    y = lax.axis_index('aux')
    x = o // 2
    c = o % 2
    par = 2 * x + (1 - c)
    far = 2 * (1 - x)

    quarter = (far + c, far + (1 - c), par, o)
    slot = (4 + c, 6, 7, c)

    def bcopy(kind, j):
        start = pl.multiple_of((quarter[kind] * CHUNKS + j) * BCH, BCH)
        return pltpu.make_async_copy(b_hbm.at[pl.ds(start, BCH)], bv.at[pl.ds(start, BCH)], bsem.at[kind, j])

    order = [(k, j) for j in range(CHUNKS) for k in (0, 1)] + [(k, j) for k in (2, 3) for j in range(CHUNKS)]
    ca_copy = pltpu.make_async_copy(ca_hbm, cav, csem.at[0])
    cb_copy = pltpu.make_async_copy(cb_hbm, cbv, csem.at[1])
    ca_copy.start()
    cb_copy.start()
    for k, j in order[:AHEAD]:
        bcopy(k, j).start()

    barrier = pltpu.get_barrier_semaphore()
    for d in range(1, 8):
        other = lax.rem(y * 4 + o + d, 8)
        pl.semaphore_signal(barrier, inc=1, device_id={'aux': other // 4, 'orb': other % 4}, device_id_type=MESH)

    ca_copy.wait()
    cb_copy.wait()
    ct[0:16, :] = cav[0:16, :]
    ct[16:32, :] = cbv[0:16, :]
    ct[32:36, :] = cav[16:20, :]
    ct[36:39, :] = cbv[16:19, :]
    ct[39:40, :] = jnp.zeros((1, NB), F32)
    cs[...] = jnp.concatenate([t.astype(F32) for t in split(ct[...])], axis=0).astype(BF16)
    own = ct[:, pl.ds(pl.multiple_of(x * 128, 128), 128)]
    turned = pltpu.roll(own, 64, 1)
    low = lax.broadcasted_iota(jnp.int32, (40, 128), 1) < 64
    own = jnp.where(low, jnp.where(c == 0, own, turned), jnp.where(c == 0, turned, own))
    crep[:, :128] = own
    crep[:, 128:] = own
    sacc[96:128, :] = jnp.zeros((32, NB), F32)

    def part(spin, s, j):
        return tb.at[spin, s, pl.ds(pl.multiple_of(j * CROWS[spin], 8), CROWS[spin])]

    def half_transform(kind, j):
        bcopy(kind, j).wait()
        first = (quarter[kind] * CHUNKS + j) * CGROUPS
        to_a = part(0, slot[kind], j)
        to_b = part(1, slot[kind], j)
        for h in range(CGROUPS // 2):
            base = pl.multiple_of((first + 2 * h) * 256, 256)
            b1, b2, b3 = split(bv[pl.ds(base, 512), :])
            r1 = dot16(cs[...], b1, ((1,), (1,)))
            r2 = dot16(cs[0:80, :], b2, ((1,), (1,)))
            r3 = dot16(cs[0:40, :], b3, ((1,), (1,)))
            r2 = ((r3 + r2[40:80] + r1[80:120]) + (r2[0:40] + r1[40:80])) + r1[0:40]
            for u in range(4):
                p = 4 * h + u
                r = r2[:, u * 128:(u + 1) * 128]
                to_a[16 * p:16 * p + 16, :] = r[0:16]
                to_b[16 * p:16 * p + 16, :] = r[16:32]
                to_a[128 + 4 * p:132 + 4 * p, :] = r[32:36]
                to_b[128 + 3 * p:131 + 3 * p, :] = r[36:39]
            for u in range(2):
                r = r2[:, u * 256:(u + 1) * 256]
                sacc[pl.ds(first + 2 * h + u, 1), :] = jnp.sum(r * crep[...], axis=0, keepdims=True)

    def remote_send(spin, kind, j):
        return pltpu.make_async_remote_copy(
            src_ref=part(spin, slot[kind], j), dst_ref=part(spin, 2 + c, j),
            send_sem=rs_s.at[spin, kind, j], recv_sem=rs_r.at[spin, c, j],
            device_id={'orb': quarter[kind]}, device_id_type=MESH)

    def remote_recv(spin, core, j):
        return pltpu.make_async_remote_copy(
            src_ref=part(spin, 2 + core, j), dst_ref=part(spin, 2 + core, j),
            send_sem=rs_s.at[spin, 0, j], recv_sem=rs_r.at[spin, core, j],
            device_id={'orb': par}, device_id_type=MESH)

    def partner_send(spin, which, j):
        return pltpu.make_async_remote_copy(
            src_ref=part(spin, 6 + which, j), dst_ref=part(spin, (4 + c) if which == 0 else c, j),
            send_sem=ps_s.at[spin, which, j], recv_sem=ps_r.at[spin, which, j],
            device_id={'orb': par}, device_id_type=MESH)

    def partner_recv(spin, which, j):
        return pltpu.make_async_remote_copy(
            src_ref=part(spin, 6, j), dst_ref=part(spin, (5 - c) if which == 0 else (1 - c), j),
            send_sem=ps_s.at[spin, which, j], recv_sem=ps_r.at[spin, which, j],
            device_id={'orb': par}, device_id_type=MESH)

    items = [(spin, k, j) for spin in range(2) for k, j in order[:2 * CHUNKS]]
    issued = [0]

    def issue(upto):
        while issued[0] < min(upto, len(items)):
            n = issued[0]
            if n >= 2 * CHUNKS:
                remote_send(*items[n - DEPTH]).wait_send()
            remote_send(*items[n]).start()
            issued[0] = n + 1

    half_transform(0, 0)
    for k, j in order[AHEAD:]:
        bcopy(k, j).start()
    pl.semaphore_wait(barrier, 7)
    issue(1)
    half_transform(1, 0)
    issue(2)
    issued[0] = 2 * CHUNKS

    def pair(j, _):
        for k in (0, 1):
            half_transform(k, j)
            remote_send(0, k, j).start()
        return 0

    lax.fori_loop(1, CHUNKS, pair, 0)

    def back(j, _):
        for spin in range(2):
            partner_send(spin, 0, j).start()
        half_transform(2, j)
        for spin in range(2):
            partner_send(spin, 1, j).start()
        return 0

    lax.fori_loop(0, CHUNKS, back, 0)

    def home(j, _):
        half_transform(3, j)
        return 0

    lax.fori_loop(0, CHUNKS - 2, home, 0)
    issue(2 * CHUNKS + 1)
    lax.fori_loop(CHUNKS - 2, CHUNKS, home, 0)
    issue(2 * CHUNKS + 2)

    e8 = (lax.broadcasted_iota(jnp.int32, (8, NB), 1) // ROWS == lax.broadcasted_iota(jnp.int32, (8, NB), 0)).astype(F32)
    gam[o] = dot(e8, sacc[...], ((1,), (1,)))

    def gamma_send(d):
        return pltpu.make_async_remote_copy(
            src_ref=gam.at[o], dst_ref=gam.at[o], send_sem=gm_s.at[d], recv_sem=gm_r.at[d],
            device_id={'orb': lax.rem(o + d, 4)}, device_id_type=MESH)

    def gamma_recv(d):
        src = lax.rem(o + 4 - d, 4)
        return pltpu.make_async_remote_copy(
            src_ref=gam.at[src], dst_ref=gam.at[src], send_sem=gm_s.at[d], recv_sem=gm_r.at[d],
            device_id={'orb': par}, device_id_type=MESH)

    for d in range(1, 4):
        gamma_send(d).start()

    def merged(spin, s, j, count=1):
        rows = count * CROWS[spin]
        at = pl.ds(pl.multiple_of(j * CROWS[spin], 8), rows)
        a = tb[spin, s, at]
        b = tb[spin, s + 1, at]
        left = lax.broadcasted_iota(jnp.int32, (rows, 128), 1) < 64
        return jnp.concatenate([jnp.where(left, a, pltpu.roll(b, 64, 1)),
                                jnp.where(left, pltpu.roll(a, 64, 1), b)], axis=0)

    zero = jnp.zeros((128, 128), F32)
    half = CHUNKS // 2
    for spin in range(2):
        acc = zero
        for which in range(2):
            def dbody(h, acc):
                for u in range(half):
                    partner_recv(spin, which, h * half + u).wait_recv()
                m = merged(spin, (4, 0)[which], h * half, half)
                return acc + dot(m, m, ((0,), (0,)))
            acc = lax.fori_loop(0, 2, dbody, acc)
            issue(issued[0] + 1)
        kd[spin, 0] = acc[:64]
        kd[spin, 1] = acc[64:]

    def block_send(src, spin, cd, xd, yd, base, sidx):
        return pltpu.make_async_remote_copy(
            src_ref=src.at[spin, cd], dst_ref=gbuf.at[spin, base + 2 * y + c],
            send_sem=gk_s.at[spin, sidx, cd], recv_sem=gk_r.at[spin, base + 2 * y + c],
            device_id={'aux': yd, 'orb': 2 * xd + cd}, device_id_type=MESH)

    def each_block(src, spin, xd, yd, base, sidx, act):
        for cd in range(2):
            mine = jnp.logical_and(jnp.logical_and(xd == x, yd == y), c == cd)

            @pl.when(jnp.logical_not(mine))
            def _():
                act(block_send(src, spin, cd, xd, yd, base, sidx))

    start = lambda copy: copy.start()
    wait_send = lambda copy: copy.wait_send()
    for spin in range(2):
        each_block(kd, spin, x, x, 0, 0, start)

    for d in range(1, 4):
        gamma_recv(d).wait_recv()
    gsum = (gam[0] + gam[1]) + (gam[2] + gam[3])
    for k in range(GRP):
        pick = (lax.broadcasted_iota(jnp.int32, (8, 128), 0) == k).astype(F32)
        grep[k] = dot(gsum, pick, ((0,), (0,)))

    def jbody(g, acc):
        for k in range(GRP):
            row = grep[k, pl.ds(g, 1), :]
            base = pl.multiple_of(g * 256 + k * ROWS, ROWS)
            acc = acc + bv[pl.ds(base, ROWS), :] * jnp.concatenate([row, row], axis=1)
        return acc

    jacc = lax.fori_loop(0, NQ // GRP, jbody, jnp.zeros((ROWS, NB), F32))
    jp[0] = jacc[:, :128]
    jp[1] = jacc[:, 128:]
    j_copy = pltpu.make_async_remote_copy(
        src_ref=jp.at[1 - y], dst_ref=jr, send_sem=j_s, recv_sem=j_r,
        device_id={'aux': 1 - y}, device_id_type=MESH)
    j_copy.start()
    issue(issued[0] + 1)

    def block_recv(spin, s):
        return pltpu.make_async_remote_copy(
            src_ref=gbuf.at[spin, s], dst_ref=gbuf.at[spin, s],
            send_sem=gk_s.at[spin, 0, 0], recv_sem=gk_r.at[spin, s],
            device_id={'orb': par}, device_id_type=MESH)

    def finish(spin, src, count):
        total = src[spin, c]
        for d in range(1, count):
            s = lax.rem(2 * y + c + d, 4) if d < 4 else d
            block_recv(spin, s).wait_recv()
            total = total + gbuf[spin, s]
        s_ref[spin * 64:spin * 64 + 64, :] = total

    for spin in range(2):
        block = zero
        for j in range(CHUNKS):
            if spin == 1:
                issue(2 * CHUNKS + 2 * j + 1 + DEPTH)
            for core in range(2):
                remote_recv(spin, core, j).wait_recv()
            block = block + dot(merged(spin, 0, j), merged(spin, 2, j), ((0,), (0,)))
        ko[spin, 0] = block[:64]
        ko[spin, 1] = block[64:]
        flip = block.T
        kot[spin, 0] = flip[:64]
        kot[spin, 1] = flip[64:]
        each_block(ko, spin, x, 1 - x, 0, 1, start)
        each_block(kot, spin, 1 - x, x, 4, 2, start)

    j_copy.wait()
    jout_ref[...] = jp[y] + jr[...]

    @pl.when(x == y)
    def _():
        finish(0, kd, 4)
        finish(1, kd, 4)

    @pl.when(x != y)
    def _():
        finish(0, ko, 8)
        finish(1, ko, 8)

    for spin in range(2):
        each_block(kd, spin, x, x, 0, 0, wait_send)
        each_block(ko, spin, x, 1 - x, 0, 1, wait_send)
        each_block(kot, spin, 1 - x, x, 4, 2, wait_send)
        for j in range(CHUNKS):
            for k in range(2):
                partner_send(spin, k, j).wait_send()
    waited = len(items) - DEPTH
    for n, item in enumerate(items):
        if n < 2 * CHUNKS - DEPTH or n >= waited:
            remote_send(*item).wait_send()
    for d in range(1, 4):
        gamma_send(d).wait_send()


def solution(mesh):
    def local_build(b_local, c_alpha, c_beta):
        b_rows = b_local.reshape(NQ * ROWS, NB)
        dma = pltpu.SemaphoreType.DMA
        vmem = pltpu.VMEM
        neg, coul = pl.pallas_call(
            kernel,
            out_shape=[pltpu.VMEM((2 * ROWS, 128), F32), pltpu.VMEM((ROWS, 128), F32)],
            in_specs=[pl.BlockSpec(memory_space=pl.ANY)] * 3,
            out_specs=[pl.BlockSpec(memory_space=vmem)] * 2,
            scratch_shapes=[
                vmem((NQ * ROWS, NB), F32),
                vmem((2, 8, TROWS, 128), F32),
                vmem((20, NB), F32), vmem((19, NB), F32),
                vmem((40, NB), F32), vmem((120, NB), BF16), vmem((40, NB), F32),
                vmem((128, NB), F32),
                vmem((4, 8, 128), F32),
                vmem((GRP, 128, 128), F32),
                vmem((2, 2, 64, 128), F32), vmem((2, 2, 64, 128), F32), vmem((2, 2, 64, 128), F32),
                vmem((2, 8, 64, 128), F32),
                vmem((2, 64, 128), F32), vmem((64, 128), F32),
                dma((4, CHUNKS)), dma((2,)),
                dma((2, 2, CHUNKS)), dma((2, 2, CHUNKS)),
                dma((2, 2, CHUNKS)), dma((2, 2, CHUNKS)),
                dma((4,)), dma((4,)),
                dma((2, 3, 2)), dma((2, 8)),
                dma, dma,
            ],
            compiler_params=pltpu.CompilerParams(
                collective_id=0, has_side_effects=True, vmem_limit_bytes=56 * 1024 * 1024),
        )(b_rows, c_alpha.T, c_beta.T)
        return coul - neg[:ROWS], coul - neg[ROWS:]

    spec_b = P(('sys', 'aux'), 'orb', None)
    spec_c = P('sys', None)
    spec_g = P(('sys', 'orb'), 'aux')
    return jax.shard_map(local_build, mesh=mesh, in_specs=(spec_b, spec_c, spec_c), out_specs=(spec_g, spec_g), check_vma=False)
```

```python
import jax
import jax.numpy as jnp
from jax import lax
from jax.experimental import pallas as pl
from jax.experimental.pallas import tpu as pltpu
from jax.sharding import PartitionSpec as P

TOP = lax.Precision.HIGHEST
MESH = pl.DeviceIdType.MESH
F32 = jnp.float32

NQ = 384
ROWS = 64
NB = 256
GRP = 4
QGROUPS = 24
CHUNKS = 6
CGROUPS = QGROUPS // CHUNKS
CROWS = (CGROUPS * 40, CGROUPS * 38)
BCH = CGROUPS * GRP * ROWS
TROWS = CHUNKS * CROWS[0]
SWITCH = 18
IA, I0, I1, I2, IT, I3, I4, I5 = 4, 4, 4, 4, 12, 14, 16, 20
AHEAD = 4
DEPTH = 8


def dot(a, b, dims):
    return lax.dot_general(a, b, (dims, ((), ())), precision=TOP, preferred_element_type=F32)


BF16 = jnp.bfloat16
SHRINK = 1.0 - 2.0 ** -9


def split(v):
    v1 = (v * SHRINK).astype(BF16)
    rest = v - v1.astype(F32)
    v2 = rest.astype(BF16)
    return v1, v2, (rest - v2.astype(F32)).astype(BF16)


def dot16(a, b, dims):
    return lax.dot_general(a, b, (dims, ((), ())), preferred_element_type=F32)


def kernel(b_hbm, ca_hbm, cb_hbm, s_ref, jout_ref,
           bv, tb, cav, cbv, ct, cs, crep, sacc, gam, grep, lt, lc, kd, kp, kt, kr, gd, gp, gt, gr, jp, jr,
           bsem, csem, rs_s, rs_r, ps_s, ps_r, gm_s, gm_r, gd_s, gd_r, gp_s, gp_r, gt_s, gt_r, gr_s, gr_r, kr_s, kr_r, j_s, j_r, turn):
    o = lax.axis_index('orb')
    y = lax.axis_index('aux')
    x = o // 2
    c = o % 2
    par = 2 * x + (1 - c)
    far = 2 * (1 - x)

    quarter = (far + c, far + (1 - c), par, o)
    slot = (4 + c, 6, 7, c)

    def bcopy(kind, j):
        start = pl.multiple_of((quarter[kind] * CHUNKS + j) * BCH, BCH)
        return pltpu.make_async_copy(b_hbm.at[pl.ds(start, BCH)], bv.at[pl.ds(start, BCH)], bsem.at[kind, j])

    order = [(k, j) for j in range(CHUNKS) for k in (0, 1)] + [(k, j) for k in (2, 3) for j in range(CHUNKS)]
    ca_copy = pltpu.make_async_copy(ca_hbm, cav, csem.at[0])
    cb_copy = pltpu.make_async_copy(cb_hbm, cbv, csem.at[1])
    ca_copy.start()
    cb_copy.start()
    for k, j in order[:AHEAD]:
        bcopy(k, j).start()

    barrier = pltpu.get_barrier_semaphore()
    def greet(yd, od):
        pl.semaphore_signal(barrier, inc=1, device_id={'aux': yd, 'orb': od}, device_id_type=MESH)

    greet(y, par)
    for od in (far, far + 1):
        greet(y, od)
    for od in (2 * x, 2 * x + 1):
        greet(1 - y, od)

    @pl.when(x != y)
    def _():
        for od in (far, far + 1):
            greet(1 - y, od)

    ca_copy.wait()
    cb_copy.wait()
    ct[0:16, :] = cav[0:16, :]
    ct[16:32, :] = cbv[0:16, :]
    ct[32:36, :] = cav[16:20, :]
    ct[36:39, :] = cbv[16:19, :]
    ct[39:40, :] = jnp.zeros((1, NB), F32)
    cs[...] = jnp.concatenate([t.astype(F32) for t in split(ct[...])], axis=0).astype(BF16)
    own = ct[:, pl.ds(pl.multiple_of(x * 128, 128), 128)]
    turned = pltpu.roll(own, 64, 1)
    low = lax.broadcasted_iota(jnp.int32, (40, 128), 1) < 64
    own = jnp.where(low, jnp.where(c == 0, own, turned), jnp.where(c == 0, turned, own))
    crep[:, :128] = own
    crep[:, 128:] = own
    sacc[96:128, :] = jnp.zeros((32, NB), F32)

    def part(spin, s, j):
        return tb.at[spin, s, pl.ds(pl.multiple_of(j * CROWS[spin], 8), CROWS[spin])]

    def half_transform(kind, j):
        bcopy(kind, j).wait()
        first = (quarter[kind] * CHUNKS + j) * CGROUPS
        to_a = part(0, slot[kind], j)
        to_b = part(1, slot[kind], j)
        for h in range(CGROUPS // 2):
            base = pl.multiple_of((first + 2 * h) * 256, 256)
            b1, b2, b3 = split(bv[pl.ds(base, 512), :])
            r1 = dot16(cs[...], b1, ((1,), (1,)))
            r2 = dot16(cs[0:80, :], b2, ((1,), (1,)))
            r3 = dot16(cs[0:40, :], b3, ((1,), (1,)))
            r2 = ((r3 + r2[40:80] + r1[80:120]) + (r2[0:40] + r1[40:80])) + r1[0:40]
            for u in range(4):
                p = 4 * h + u
                r = r2[:, u * 128:(u + 1) * 128]
                to_a[16 * p:16 * p + 16, :] = r[0:16]
                to_b[16 * p:16 * p + 16, :] = r[16:32]
                to_a[128 + 4 * p:132 + 4 * p, :] = r[32:36]
                to_b[128 + 3 * p:131 + 3 * p, :] = r[36:39]
            for u in range(2):
                r = r2[:, u * 256:(u + 1) * 256]
                sacc[pl.ds(first + 2 * h + u, 1), :] = jnp.sum(r * crep[...], axis=0, keepdims=True)

    def remote_send(spin, kind, j):
        return pltpu.make_async_remote_copy(
            src_ref=part(spin, slot[kind], j), dst_ref=part(spin, 2 + c, j),
            send_sem=rs_s.at[spin, kind, j], recv_sem=rs_r.at[spin, c, j],
            device_id={'orb': quarter[kind]}, device_id_type=MESH)

    def partner_send(spin, which, j):
        return pltpu.make_async_remote_copy(
            src_ref=part(spin, 6 + which, j), dst_ref=part(spin, (4 + c) if which == 0 else c, j),
            send_sem=ps_s.at[spin, which, j], recv_sem=ps_r.at[spin, which, j],
            device_id={'orb': par}, device_id_type=MESH)

    def partner_recv(spin, which, j):
        return pltpu.make_async_remote_copy(
            src_ref=part(spin, 6, j), dst_ref=part(spin, (5 - c) if which == 0 else (1 - c), j),
            send_sem=ps_s.at[spin, which, j], recv_sem=ps_r.at[spin, which, j],
            device_id={'orb': par}, device_id_type=MESH)

    items = [(spin, k, j) for spin in range(2) for k, j in order[:2 * CHUNKS]]
    turns = [(spin, k, j) for spin in range(2) for j in range(CHUNKS) for k in (1, 0)]
    turns = turns[:-4] + sorted(turns[-4:], key=lambda item: -item[1])
    issued = [0]

    def issue(upto):
        todo = range(issued[0], min(upto, len(turns)))
        issued[0] = max(issued[0], min(upto, len(turns)))

        @pl.when(c == 1)
        def _():
            for n in todo:
                if n >= DEPTH:
                    remote_send(*turns[n - DEPTH]).wait_send()
                remote_send(*turns[n]).start()

    half_transform(0, 0)
    for k, j in order[AHEAD:]:
        bcopy(k, j).start()
    pl.semaphore_wait(barrier, jnp.where(x == y, 5, 7))

    @pl.when(c == 0)
    def _():
        remote_send(0, 0, 0).start()

    half_transform(1, 0)

    @pl.when(c == 0)
    def _():
        remote_send(0, 1, 0).start()

    def pair(j, _):
        for k in (0, 1):
            half_transform(k, j)

            @pl.when(c == 0)
            def _():
                remote_send(0, k, j).start()
        for spin in range(2):
            partner_send(spin, 0, j).start()
        return 0

    for spin in range(2):
        partner_send(spin, 0, 0).start()
    lax.fori_loop(1, CHUNKS, pair, 0)
    issue(IA)

    def back(j, _):
        half_transform(2, j)
        for spin in range(2):
            partner_send(spin, 1, j).start()
        return 0

    lax.fori_loop(0, CHUNKS, back, 0)

    @pl.when(c == 0)
    def _():
        for item in items[2 * CHUNKS:]:
            remote_send(*item).start()

    def home(j, _):
        half_transform(3, j)
        return 0

    lax.fori_loop(0, CHUNKS, home, 0)
    issue(I0)

    e8 = (lax.broadcasted_iota(jnp.int32, (8, NB), 1) // ROWS == lax.broadcasted_iota(jnp.int32, (8, NB), 0)).astype(F32)
    gam[o] = dot(e8, sacc[...], ((1,), (1,)))

    def gamma_send(d):
        return pltpu.make_async_remote_copy(
            src_ref=gam.at[o], dst_ref=gam.at[o], send_sem=gm_s.at[d], recv_sem=gm_r.at[d],
            device_id={'orb': lax.rem(o + d, 4)}, device_id_type=MESH)

    def gamma_recv(d):
        src = lax.rem(o + 4 - d, 4)
        return pltpu.make_async_remote_copy(
            src_ref=gam.at[src], dst_ref=gam.at[src], send_sem=gm_s.at[d], recv_sem=gm_r.at[d],
            device_id={'orb': par}, device_id_type=MESH)

    for d in range(1, 4):
        gamma_send(d).start()

    def sides(spin, s, j, count):
        rows = count * CROWS[spin]
        at = pl.ds(pl.multiple_of(j * CROWS[spin], 8), rows)
        a = tb[spin, s, at]
        b = tb[spin, s + 1, at]
        left = lax.broadcasted_iota(jnp.int32, (rows, 128), 1) < 64
        return jnp.where(left, a, pltpu.roll(b, 64, 1)), jnp.where(left, pltpu.roll(a, 64, 1), b)

    half = CHUNKS // 2
    for spin in range(2):
        cols = 2 * half * CROWS[spin]
        acc = (jnp.zeros((128, 128), F32),) * 2
        for which in range(2):
            def dbody(h, acc):
                for u in range(half):
                    partner_recv(spin, which, h * half + u).wait_recv()
                m = jnp.concatenate(sides(spin, (4, 0)[which], h * half, half), axis=0)
                m1, m2, m3 = split(m)
                t1, t2, t3 = split(m.T)
                r = dot16(jnp.concatenate([t1, t2], axis=0), jnp.concatenate([m1, m2], axis=1), ((1,), (0,)))
                q = dot16(t1, m3, ((1,), (0,)))
                if which == 1:
                    lt[spin, h, :, 0:cols] = jnp.concatenate([t1, t2, t3], axis=0)
                return acc[0] + ((r[128:, 128:] + (r[:128, 128:] + r[128:, :128])) + r[:128, :128]), acc[1] + q
            acc = lax.fori_loop(0, 2, dbody, acc)
        acc = acc[0] + (acc[1] + acc[1].T)
        kd[spin, 0] = acc[:64]
        kd[spin, 1] = acc[64:]
        if spin == 1:
            for u in range(half):
                lc[u, :, 0:2 * CROWS[1]] = jnp.concatenate(split(jnp.concatenate(sides(1, 0, half + u, 1), axis=0).T), axis=0)
        issue(I1 if spin == 0 else I2)

    def kd_send(spin, cd):
        return pltpu.make_async_remote_copy(
            src_ref=kd.at[spin, cd], dst_ref=gd.at[spin, 2 * y + c],
            send_sem=gd_s.at[spin, cd], recv_sem=gd_r.at[spin, 2 * y + c],
            device_id={'aux': x, 'orb': 2 * x + cd}, device_id_type=MESH)

    def kp_send(spin, cs, cd):
        return pltpu.make_async_remote_copy(
            src_ref=kp.at[spin, cs, cd], dst_ref=gp.at[spin, cs, 2 * y + c],
            send_sem=gp_s.at[spin, cs, cd], recv_sem=gp_r.at[spin, cs, 2 * y + c],
            device_id={'aux': 1 - x, 'orb': 2 * x + cd}, device_id_type=MESH)

    def kt_send(spin):
        return pltpu.make_async_remote_copy(
            src_ref=kt.at[spin, 1], dst_ref=gt.at[2 * y + c],
            send_sem=gt_s, recv_sem=gt_r.at[2 * y + c],
            device_id={'aux': x, 'orb': 2 * (1 - x) + 1}, device_id_type=MESH)

    def gr_send(spin, cs):
        return pltpu.make_async_remote_copy(
            src_ref=kt.at[spin, cs], dst_ref=gr.at[spin, 2 * y + c],
            send_sem=gr_s.at[spin, cs], recv_sem=gr_r.at[spin, 2 * y + c],
            device_id={'aux': 0, 'orb': 2 * x + cs}, device_id_type=MESH)

    def kr_send(spin, cs):
        return pltpu.make_async_remote_copy(
            src_ref=kr.at[spin, 0], dst_ref=kr.at[spin, 1],
            send_sem=kr_s.at[spin], recv_sem=kr_r.at[spin],
            device_id={'aux': x, 'orb': 2 * (1 - x) + cs}, device_id_type=MESH)

    def relay(spin, cs):
        @pl.when(jnp.logical_and(y == 0, c == cs))
        def _():
            total = kt[spin, cs]
            for d in range(1, 4):
                s = lax.rem(2 * y + c + d, 4)
                landed(gr.at[spin, s], gr_r.at[spin, s])
                total = total + gr[spin, s]
            kr[spin, 0] = total
            kr_send(spin, cs).start()

    def landed(dst, sem):
        return pltpu.make_async_remote_copy(
            src_ref=dst, dst_ref=dst, send_sem=j_s, recv_sem=sem, device_id={'orb': par}, device_id_type=MESH).wait_recv()

    start = lambda copy: copy.start()
    wait_send = lambda copy: copy.wait_send()

    def each_kd(spin, act):
        for cd in range(2):
            @pl.when(jnp.logical_not(jnp.logical_and(x == y, c == cd)))
            def _():
                act(kd_send(spin, cd))

    def each_ko(spin, cs, act):
        if (spin, cs) == (1, 1):
            act(kt_send(spin))
        else:
            @pl.when(jnp.logical_not(jnp.logical_and(y == 0, c == cs)))
            def _():
                act(gr_send(spin, cs))
        for cd in range(2):
            @pl.when(jnp.logical_not(jnp.logical_and(x != y, c == cd)))
            def _():
                act(kp_send(spin, cs, cd))

    for spin in range(2):
        each_kd(spin, start)

    @pl.when(c == 0)
    def _():
        for item in items[:SWITCH]:
            remote_send(*item).wait_send()
        pl.semaphore_signal(turn, inc=1, device_id={'orb': par}, device_id_type=MESH)

    @pl.when(c == 1)
    def _():
        pl.semaphore_wait(turn, 1)

    issue(IT)

    def off_part(spin, cs, j, count, left_side, acc):
        for u in range(count):
            landed(part(spin, 2 + cs, j + u), rs_r.at[spin, cs, j + u])
        rows = count * CROWS[spin]
        v = tb[spin, 2 + cs, j * CROWS[spin]:j * CROWS[spin] + rows]
        v1, v2, v3 = [t.astype(F32) for t in split(v)]
        left = lax.broadcasted_iota(jnp.int32, (rows, 128), 1) < 64
        none = jnp.zeros((rows, 128), F32)
        w = jnp.concatenate([
            jnp.concatenate([jnp.where(left, v1, pltpu.roll(v2, 64, 1)), jnp.where(left, v3, none)], axis=1),
            jnp.concatenate([jnp.where(left, pltpu.roll(v1, 64, 1), v2), jnp.where(left, pltpu.roll(v3, 64, 1), none)], axis=1),
        ], axis=0).astype(BF16)
        r = dot16(left_side[:, 0:2 * rows], w, ((1,), (0,)))
        return acc + ((r[256:] + r[128:256]) + r[:128])

    def off_done(spin, cs, acc):
        block = acc[:, :128] + acc[:, 128:]
        block = block + pltpu.roll(block, 64, 1)
        left = lax.broadcasted_iota(jnp.int32, (32, 128), 1) < 64
        for cd in range(2):
            kp[spin, cs, cd] = jnp.where(left, block[64 * cd:64 * cd + 32], pltpu.roll(block[64 * cd + 32:64 * cd + 64], 64, 1))
        kt[spin, cs] = block.T[:64]
        each_ko(spin, cs, start)

    zero = jnp.zeros((128, NB), F32)
    for spin in range(2):
        acc = zero
        for h in range(2):
            acc = off_part(spin, 0, h * half, half, lt.at[spin, h], acc)
        off_done(spin, 0, acc)
        issue(I3 if spin == 0 else I4)
        if spin == 1:
            relay(0, 0)

    for d in range(1, 4):
        gamma_recv(d).wait_recv()
    gsum = (gam[0] + gam[1]) + (gam[2] + gam[3])
    for k in range(GRP):
        pick = (lax.broadcasted_iota(jnp.int32, (8, 128), 0) == k).astype(F32)
        grep[k] = dot(gsum, pick, ((0,), (0,)))

    def jbody(g, acc):
        for k in range(GRP):
            row = grep[k, pl.ds(g, 1), :]
            base = pl.multiple_of(g * 256 + k * ROWS, ROWS)
            acc = acc + bv[pl.ds(base, ROWS), :] * jnp.concatenate([row, row], axis=1)
        return acc

    jacc = lax.fori_loop(0, NQ // GRP, jbody, jnp.zeros((ROWS, NB), F32))
    jp[0] = jacc[:, :128]
    jp[1] = jacc[:, 128:]
    j_copy = pltpu.make_async_remote_copy(
        src_ref=jp.at[1 - y], dst_ref=jr, send_sem=j_s, recv_sem=j_r,
        device_id={'aux': 1 - y}, device_id_type=MESH)
    j_copy.start()
    issue(I5)

    relay(1, 0)

    acc = zero
    for h in range(2):
        issue(2 * (h + 1) * half + DEPTH - 1)
        acc = off_part(0, 1, h * half, half, lt.at[0, h], acc)
    off_done(0, 1, acc)

    def finish_kd(spin):
        total = kd[spin, c]
        for d in range(1, 4):
            s = lax.rem(2 * y + c + d, 4)
            landed(gd.at[spin, s], gd_r.at[spin, s])
            total = total + gd[spin, s]
        s_ref[spin * 64:spin * 64 + 64, :] = total

    def finish_ko(spin):
        pair_sum = []
        for cs in range(2):
            total = kp[spin, cs, c]
            for d in range(1, 4):
                s = lax.rem(2 * y + c + d, 4)
                landed(gp.at[spin, cs, s], gp_r.at[spin, cs, s])
                total = total + gp[spin, cs, s]
            pair_sum.append(total)
        if spin == 0:
            landed(kr.at[0, 1], kr_r.at[0])
            turned = kr[0, 1]
        else:
            @pl.when(c == 0)
            def _():
                landed(kr.at[1, 1], kr_r.at[1])

            @pl.when(c == 1)
            def _():
                for s in range(4):
                    landed(gt.at[s], gt_r.at[s])
                kr[1, 1] = (gt[0] + gt[1]) + (gt[2] + gt[3])
            turned = kr[1, 1]
        a, b = pair_sum
        left = lax.broadcasted_iota(jnp.int32, (32, 128), 1) < 64
        s_ref[spin * 64:spin * 64 + 32, :] = turned[:32] + jnp.where(left, a, pltpu.roll(b, 64, 1))
        s_ref[spin * 64 + 32:spin * 64 + 64, :] = turned[32:] + jnp.where(left, pltpu.roll(a, 64, 1), b)

    acc = zero
    for j, count in ((0, half), (half, 1), (half + 1, 1), (half + 2, 1)):
        issue(2 * (CHUNKS + j + count) + DEPTH)
        acc = off_part(1, 1, j, count, lt.at[1, 0] if j == 0 else lc.at[j - half], acc)
        if j == 0:
            relay(0, 1)
            j_copy.wait()
            jout_ref[...] = jp[y] + jr[...]

            @pl.when(x == y)
            def _():
                finish_kd(0)
                finish_kd(1)

            @pl.when(x != y)
            def _():
                finish_ko(0)
    off_done(1, 1, acc)

    @pl.when(x != y)
    def _():
        finish_ko(1)

    for spin in range(2):
        each_kd(spin, wait_send)
        for cs in range(2):
            each_ko(spin, cs, wait_send)
        for j in range(CHUNKS):
            for k in range(2):
                partner_send(spin, k, j).wait_send()

    @pl.when(c == 0)
    def _():
        for item in items[SWITCH:]:
            remote_send(*item).wait_send()

    @pl.when(c == 1)
    def _():
        for item in turns[-DEPTH:]:
            remote_send(*item).wait_send()

    for spin, cs in ((0, 0), (1, 0), (0, 1)):
        @pl.when(jnp.logical_and(y == 0, c == cs))
        def _():
            kr_send(spin, cs).wait_send()

    for d in range(1, 4):
        gamma_send(d).wait_send()


def solution(mesh):
    def local_build(b_local, c_alpha, c_beta):
        b_rows = b_local.reshape(NQ * ROWS, NB)
        dma = pltpu.SemaphoreType.DMA
        vmem = pltpu.VMEM
        neg, coul = pl.pallas_call(
            kernel,
            out_shape=[pltpu.VMEM((2 * ROWS, 128), F32), pltpu.VMEM((ROWS, 128), F32)],
            in_specs=[pl.BlockSpec(memory_space=pl.ANY)] * 3,
            out_specs=[pl.BlockSpec(memory_space=vmem)] * 2,
            scratch_shapes=[
                vmem((NQ * ROWS, NB), F32),
                vmem((2, 8, TROWS, 128), F32),
                vmem((20, NB), F32), vmem((19, NB), F32),
                vmem((40, NB), F32), vmem((120, NB), BF16), vmem((40, NB), F32),
                vmem((128, NB), F32),
                vmem((4, 8, 128), F32),
                vmem((GRP, 128, 128), F32),
                vmem((2, 2, 384, CHUNKS * CROWS[0]), BF16),
                vmem((CHUNKS // 2, 384, 384), BF16),
                vmem((2, 2, 64, 128), F32), vmem((2, 2, 2, 32, 128), F32), vmem((2, 2, 64, 128), F32),
                vmem((2, 2, 64, 128), F32),
                vmem((2, 4, 64, 128), F32), vmem((2, 2, 4, 32, 128), F32), vmem((4, 64, 128), F32),
                vmem((2, 4, 64, 128), F32),
                vmem((2, 64, 128), F32), vmem((64, 128), F32),
                dma((4, CHUNKS)), dma((2,)),
                dma((2, 2, CHUNKS)), dma((2, 2, CHUNKS)),
                dma((2, 2, CHUNKS)), dma((2, 2, CHUNKS)),
                dma((4,)), dma((4,)),
                dma((2, 2)), dma((2, 4)), dma((2, 2, 2)), dma((2, 2, 4)), dma, dma((4,)),
                dma((2, 2)), dma((2, 4)), dma((2,)), dma((2,)),
                dma, dma, pltpu.SemaphoreType.REGULAR,
            ],
            compiler_params=pltpu.CompilerParams(
                collective_id=0, has_side_effects=True, vmem_limit_bytes=56 * 1024 * 1024),
        )(b_rows, c_alpha.T, c_beta.T)
        return coul - neg[:ROWS], coul - neg[ROWS:]

    spec_b = P(('sys', 'aux'), 'orb', None)
    spec_c = P('sys', None)
    spec_g = P(('sys', 'orb'), 'aux')
    return jax.shard_map(local_build, mesh=mesh, in_specs=(spec_b, spec_c, spec_c), out_specs=(spec_g, spec_g), check_vma=False)
```

```python
import jax
import jax.numpy as jnp
from jax import lax
from jax.experimental import pallas as pl
from jax.experimental.pallas import tpu as pltpu
from jax.sharding import PartitionSpec as P

TOP = lax.Precision.HIGHEST
MESH = pl.DeviceIdType.MESH
F32 = jnp.float32

NQ = 384
ROWS = 64
NB = 256
GRP = 4
QGROUPS = 24
CHUNKS = 6
CGROUPS = QGROUPS // CHUNKS
CROWS = (CGROUPS * 40, CGROUPS * 38)
BCH = CGROUPS * GRP * ROWS
TROWS = CHUNKS * CROWS[0]
SWITCH = 14
LAST = ((1, 3), (0, 3), (1, 4), (1, 5), (0, 4), (0, 5))
IA, I0, I1, I2, IT, I3, I4, I5 = 1, 1, 1, 1, 4, 4, 5, 6
AHEAD = 4
DEPTH = 6


def dot(a, b, dims):
    return lax.dot_general(a, b, (dims, ((), ())), precision=TOP, preferred_element_type=F32)


BF16 = jnp.bfloat16
SHRINK = 1.0 - 2.0 ** -9


def split(v):
    v1 = (v * SHRINK).astype(BF16)
    rest = v - v1.astype(F32)
    v2 = rest.astype(BF16)
    return v1, v2, (rest - v2.astype(F32)).astype(BF16)


def dot16(a, b, dims):
    return lax.dot_general(a, b, (dims, ((), ())), preferred_element_type=F32)


def kernel(b_hbm, ca_hbm, cb_hbm, s_ref, jout_ref,
           bv, tb, cav, cbv, ct, cs, crep, sacc, gam, grep, lt, lc, kd, kp, kt, kr, gd, gp, gt, gr, jp, jr,
           bsem, csem, rs_s, rs_r, ps_s, ps_r, gm_s, gm_r, gd_s, gd_r, gp_s, gp_r, gt_s, gt_r, gr_s, gr_r, kr_s, kr_r, j_s, j_r, turn):
    o = lax.axis_index('orb')
    y = lax.axis_index('aux')
    x = o // 2
    c = o % 2
    par = 2 * x + (1 - c)
    far = 2 * (1 - x)

    quarter = (far + c, far + (1 - c), par, o)
    slot = (4 + c, 6, 7, c)

    def bcopy(kind, j):
        start = pl.multiple_of((quarter[kind] * CHUNKS + j) * BCH, BCH)
        return pltpu.make_async_copy(b_hbm.at[pl.ds(start, BCH)], bv.at[pl.ds(start, BCH)], bsem.at[kind, j])

    order = [(k, j) for j in range(CHUNKS) for k in (0, 1)] + [(k, j) for k in (2, 3) for j in range(CHUNKS)]
    ca_copy = pltpu.make_async_copy(ca_hbm, cav, csem.at[0])
    cb_copy = pltpu.make_async_copy(cb_hbm, cbv, csem.at[1])
    def bpiece(kind, j, u):
        rows = BCH // 4
        start = pl.multiple_of((quarter[kind] * CHUNKS + j) * BCH + u * rows, rows)
        return pltpu.make_async_copy(b_hbm.at[pl.ds(start, rows)], bv.at[pl.ds(start, rows)], bsem.at[kind, j])

    for u in range(4):
        bpiece(0, 0, u).start()
    ca_copy.start()
    cb_copy.start()
    for k, j in order[1:1]:
        for u in range(4):
            bpiece(k, j, u).start()
    for k, j in order[1:AHEAD]:
        bcopy(k, j).start()

    barrier = pltpu.get_barrier_semaphore()
    def greet(yd, od):
        pl.semaphore_signal(barrier, inc=1, device_id={'aux': yd, 'orb': od}, device_id_type=MESH)

    greet(y, par)
    for od in (far, far + 1):
        greet(y, od)
    for od in (2 * x, 2 * x + 1):
        greet(1 - y, od)

    @pl.when(x != y)
    def _():
        for od in (far, far + 1):
            greet(1 - y, od)

    ca_copy.wait()
    cb_copy.wait()
    ct[0:16, :] = cav[0:16, :]
    ct[16:32, :] = cbv[0:16, :]
    ct[32:36, :] = cav[16:20, :]
    ct[36:39, :] = cbv[16:19, :]
    ct[39:40, :] = jnp.zeros((1, NB), F32)
    cs[...] = jnp.concatenate([t.astype(F32) for t in split(ct[...])], axis=0).astype(BF16)
    own = ct[:, pl.ds(pl.multiple_of(x * 128, 128), 128)]
    turned = pltpu.roll(own, 64, 1)
    low = lax.broadcasted_iota(jnp.int32, (40, 128), 1) < 64
    own = jnp.where(low, jnp.where(c == 0, own, turned), jnp.where(c == 0, turned, own))
    crep[:, :128] = own
    crep[:, 128:] = own
    sacc[96:128, :] = jnp.zeros((32, NB), F32)

    def part(spin, s, j, count=1):
        return tb.at[spin, s, pl.ds(pl.multiple_of(j * CROWS[spin], 8), count * CROWS[spin])]

    def half_transform(kind, j):
        bcopy(kind, j).wait()
        first = (quarter[kind] * CHUNKS + j) * CGROUPS
        to_a = part(0, slot[kind], j)
        to_b = part(1, slot[kind], j)
        for h in range(CGROUPS // 2):
            base = pl.multiple_of((first + 2 * h) * 256, 256)
            b1, b2, b3 = split(bv[pl.ds(base, 512), :])
            r1 = dot16(cs[...], b1, ((1,), (1,)))
            r2 = dot16(cs[0:80, :], b2, ((1,), (1,)))
            r3 = dot16(cs[0:40, :], b3, ((1,), (1,)))
            r2 = ((r3 + r2[40:80] + r1[80:120]) + (r2[0:40] + r1[40:80])) + r1[0:40]
            for u in range(4):
                p = 4 * h + u
                r = r2[:, u * 128:(u + 1) * 128]
                to_a[16 * p:16 * p + 16, :] = r[0:16]
                to_b[16 * p:16 * p + 16, :] = r[16:32]
                to_a[128 + 4 * p:132 + 4 * p, :] = r[32:36]
                to_b[128 + 3 * p:131 + 3 * p, :] = r[36:39]
            for u in range(2):
                r = r2[:, u * 256:(u + 1) * 256]
                sacc[pl.ds(first + 2 * h + u, 1), :] = jnp.sum(r * crep[...], axis=0, keepdims=True)

    def remote_send(spin, kind, j, count=1):
        return pltpu.make_async_remote_copy(
            src_ref=part(spin, slot[kind], j, count), dst_ref=part(spin, 2 + c, j, count),
            send_sem=rs_s.at[spin, kind, j], recv_sem=rs_r.at[spin, c, j],
            device_id={'orb': quarter[kind]}, device_id_type=MESH)

    def partner_send(spin, which, j):
        return pltpu.make_async_remote_copy(
            src_ref=part(spin, 6 + which, j), dst_ref=part(spin, (4 + c) if which == 0 else c, j),
            send_sem=ps_s.at[spin, which, j], recv_sem=ps_r.at[spin, which, j],
            device_id={'orb': par}, device_id_type=MESH)

    def partner_recv(spin, which, j):
        return pltpu.make_async_remote_copy(
            src_ref=part(spin, 6, j), dst_ref=part(spin, (5 - c) if which == 0 else (1 - c), j),
            send_sem=ps_s.at[spin, which, j], recv_sem=ps_r.at[spin, which, j],
            device_id={'orb': par}, device_id_type=MESH)

    half = CHUNKS // 2
    items = [(0, k, j, 1) for k, j in order[:2 * CHUNKS]] + [(1, k, j, half) for j in (0, half) for k in (0, 1)]
    turns = [(0, k, j, half) for j in (0, half) for k in (1, 0)] + [(1, k, 0, half) for k in (1, 0)]
    turns += [(1, k, j, 1) for k, j in LAST]
    issued = [0]
    issued = [0]

    def issue(upto):
        todo = range(issued[0], min(upto, len(turns)))
        issued[0] = max(issued[0], min(upto, len(turns)))

        @pl.when(c == 1)
        def _():
            for n in todo:
                if n >= DEPTH:
                    remote_send(*turns[n - DEPTH]).wait_send()
                remote_send(*turns[n]).start()

    half_transform(0, 0)
    for k, j in order[AHEAD:]:
        bcopy(k, j).start()
    pl.semaphore_wait(barrier, jnp.where(x == y, 5, 7))

    @pl.when(c == 0)
    def _():
        remote_send(0, 0, 0).start()

    half_transform(1, 0)

    @pl.when(c == 0)
    def _():
        remote_send(0, 1, 0).start()

    def pair(j, _):
        for k in (0, 1):
            half_transform(k, j)

            @pl.when(c == 0)
            def _():
                remote_send(0, k, j).start()
        for spin in range(2):
            partner_send(spin, 0, j).start()
        return 0

    for spin in range(2):
        partner_send(spin, 0, 0).start()
    lax.fori_loop(1, CHUNKS, pair, 0)
    issue(IA)

    def back(j, _):
        half_transform(2, j)
        for spin in range(2):
            partner_send(spin, 1, j).start()
        return 0

    lax.fori_loop(0, CHUNKS, back, 0)

    @pl.when(c == 0)
    def _():
        for item in items[2 * CHUNKS:]:
            remote_send(*item).start()

    def home(j, _):
        half_transform(3, j)
        return 0

    lax.fori_loop(0, CHUNKS, home, 0)
    issue(I0)

    e8 = (lax.broadcasted_iota(jnp.int32, (8, NB), 1) // ROWS == lax.broadcasted_iota(jnp.int32, (8, NB), 0)).astype(F32)
    gam[o] = dot(e8, sacc[...], ((1,), (1,)))

    def gamma_send(d):
        return pltpu.make_async_remote_copy(
            src_ref=gam.at[o], dst_ref=gam.at[o], send_sem=gm_s.at[d], recv_sem=gm_r.at[d],
            device_id={'orb': lax.rem(o + d, 4)}, device_id_type=MESH)

    def gamma_recv(d):
        src = lax.rem(o + 4 - d, 4)
        return pltpu.make_async_remote_copy(
            src_ref=gam.at[src], dst_ref=gam.at[src], send_sem=gm_s.at[d], recv_sem=gm_r.at[d],
            device_id={'orb': par}, device_id_type=MESH)

    for d in range(1, 4):
        gamma_send(d).start()

    def sides(spin, s, j, count):
        rows = count * CROWS[spin]
        at = pl.ds(pl.multiple_of(j * CROWS[spin], 8), rows)
        a = tb[spin, s, at]
        b = tb[spin, s + 1, at]
        left = lax.broadcasted_iota(jnp.int32, (rows, 128), 1) < 64
        return jnp.where(left, a, pltpu.roll(b, 64, 1)), jnp.where(left, pltpu.roll(a, 64, 1), b)

    for spin in range(2):
        cols = 2 * half * CROWS[spin]
        acc = (jnp.zeros((128, 128), F32),) * 2
        for which in range(2):
            def dbody(h, acc):
                for u in range(half):
                    partner_recv(spin, which, h * half + u).wait_recv()
                m = jnp.concatenate(sides(spin, (4, 0)[which], h * half, half), axis=0)
                m1, m2, m3 = split(m)
                t1, t2, t3 = split(m.T)
                r = dot16(jnp.concatenate([t1, t2], axis=0), jnp.concatenate([m1, m2], axis=1), ((1,), (0,)))
                q = dot16(t1, m3, ((1,), (0,)))
                if which == 1:
                    lt[spin, h, :, 0:cols] = jnp.concatenate([t1, t2, t3], axis=0)
                return acc[0] + ((r[128:, 128:] + (r[:128, 128:] + r[128:, :128])) + r[:128, :128]), acc[1] + q
            acc = lax.fori_loop(0, 2, dbody, acc)
        acc = acc[0] + (acc[1] + acc[1].T)
        kd[spin, 0] = acc[:64]
        kd[spin, 1] = acc[64:]
        if spin == 1:
            for u in range(half):
                lc[u, :, 0:2 * CROWS[1]] = jnp.concatenate(split(jnp.concatenate(sides(1, 0, half + u, 1), axis=0).T), axis=0)
        issue(I1 if spin == 0 else I2)

    def kd_send(spin, cd):
        return pltpu.make_async_remote_copy(
            src_ref=kd.at[spin, cd], dst_ref=gd.at[spin, 2 * y + c],
            send_sem=gd_s.at[spin, cd], recv_sem=gd_r.at[spin, 2 * y + c],
            device_id={'aux': x, 'orb': 2 * x + cd}, device_id_type=MESH)

    def kp_send(spin, cs, cd):
        return pltpu.make_async_remote_copy(
            src_ref=kp.at[spin, cs, cd], dst_ref=gp.at[spin, cs, 2 * y + c],
            send_sem=gp_s.at[spin, cs, cd], recv_sem=gp_r.at[spin, cs, 2 * y + c],
            device_id={'aux': 1 - x, 'orb': 2 * x + cd}, device_id_type=MESH)

    def kt_send(spin):
        return pltpu.make_async_remote_copy(
            src_ref=kt.at[spin, 1], dst_ref=gt.at[2 * y + c],
            send_sem=gt_s, recv_sem=gt_r.at[2 * y + c],
            device_id={'aux': x, 'orb': 2 * (1 - x) + 1}, device_id_type=MESH)

    def hub(spin, cs):
        return x if (spin, cs) in ((0, 0), (1, 0)) else 0

    def gr_send(spin, cs):
        return pltpu.make_async_remote_copy(
            src_ref=kt.at[spin, cs], dst_ref=gr.at[spin, 2 * y + c],
            send_sem=gr_s.at[spin, cs], recv_sem=gr_r.at[spin, 2 * y + c],
            device_id={'aux': hub(spin, cs), 'orb': 2 * x + cs}, device_id_type=MESH)

    def kr_send(spin, cs):
        return pltpu.make_async_remote_copy(
            src_ref=kr.at[spin, 0], dst_ref=kr.at[spin, 1],
            send_sem=kr_s.at[spin], recv_sem=kr_r.at[spin],
            device_id={'aux': x, 'orb': 2 * (1 - x) + cs}, device_id_type=MESH)

    def relay(spin, cs):
        @pl.when(jnp.logical_and(y == hub(spin, cs), c == cs))
        def _():
            total = kt[spin, cs]
            for d in range(1, 4):
                s = lax.rem(2 * y + c + d, 4)
                landed(gr.at[spin, s], gr_r.at[spin, s])
                total = total + gr[spin, s]
            kr[spin, 0] = total
            kr_send(spin, cs).start()

    def landed(dst, sem):
        return pltpu.make_async_remote_copy(
            src_ref=dst, dst_ref=dst, send_sem=j_s, recv_sem=sem, device_id={'orb': par}, device_id_type=MESH).wait_recv()

    start = lambda copy: copy.start()
    wait_send = lambda copy: copy.wait_send()

    def each_kd(spin, act):
        for cd in range(2):
            @pl.when(jnp.logical_not(jnp.logical_and(x == y, c == cd)))
            def _():
                act(kd_send(spin, cd))

    def each_ko(spin, cs, act):
        if (spin, cs) == (1, 1):
            act(kt_send(spin))
        else:
            @pl.when(jnp.logical_not(jnp.logical_and(y == hub(spin, cs), c == cs)))
            def _():
                act(gr_send(spin, cs))
        for cd in range(2):
            @pl.when(jnp.logical_not(jnp.logical_and(x != y, c == cd)))
            def _():
                act(kp_send(spin, cs, cd))

    for spin in range(2):
        each_kd(spin, start)

    @pl.when(c == 0)
    def _():
        for item in items[:SWITCH]:
            remote_send(*item).wait_send()
        pl.semaphore_signal(turn, inc=1, device_id={'orb': par}, device_id_type=MESH)

    @pl.when(c == 1)
    def _():
        pl.semaphore_wait(turn, 1)

    issue(IT)

    def off_part(spin, cs, j, count, left_side, acc):
        step = 1 if (spin, cs) == (0, 0) else count
        for u in range(0, count, step):
            landed(part(spin, 2 + cs, j + u, step), rs_r.at[spin, cs, j + u])
        rows = count * CROWS[spin]
        v = tb[spin, 2 + cs, j * CROWS[spin]:j * CROWS[spin] + rows]
        v1, v2, v3 = [t.astype(F32) for t in split(v)]
        left = lax.broadcasted_iota(jnp.int32, (rows, 128), 1) < 64
        none = jnp.zeros((rows, 128), F32)
        w = jnp.concatenate([
            jnp.concatenate([jnp.where(left, v1, pltpu.roll(v2, 64, 1)), jnp.where(left, v3, none)], axis=1),
            jnp.concatenate([jnp.where(left, pltpu.roll(v1, 64, 1), v2), jnp.where(left, pltpu.roll(v3, 64, 1), none)], axis=1),
        ], axis=0).astype(BF16)
        r = dot16(left_side[:, 0:2 * rows], w, ((1,), (0,)))
        return acc + ((r[256:] + r[128:256]) + r[:128])

    def off_done(spin, cs, acc):
        block = acc[:, :128] + acc[:, 128:]
        block = block + pltpu.roll(block, 64, 1)
        left = lax.broadcasted_iota(jnp.int32, (32, 128), 1) < 64
        kt[spin, cs] = block.T[:64]
        for cd in range(2):
            kp[spin, cs, cd] = jnp.where(left, block[64 * cd:64 * cd + 32], pltpu.roll(block[64 * cd + 32:64 * cd + 64], 64, 1))
        each_ko(spin, cs, start)

    zero = jnp.zeros((128, NB), F32)
    for spin in range(2):
        acc = zero
        for h in range(2):
            acc = off_part(spin, 0, h * half, half, lt.at[spin, h], acc)
        off_done(spin, 0, acc)
        issue(I3 if spin == 0 else I4)
        if spin == 1:
            relay(0, 0)

    for d in range(1, 4):
        gamma_recv(d).wait_recv()
    gsum = (gam[0] + gam[1]) + (gam[2] + gam[3])
    for k in range(GRP):
        pick = (lax.broadcasted_iota(jnp.int32, (8, 128), 0) == k).astype(F32)
        grep[k] = dot(gsum, pick, ((0,), (0,)))

    def jbody(g, acc):
        for k in range(GRP):
            row = grep[k, pl.ds(g, 1), :]
            base = pl.multiple_of(g * 256 + k * ROWS, ROWS)
            acc = acc + bv[pl.ds(base, ROWS), :] * jnp.concatenate([row, row], axis=1)
        return acc

    jacc = lax.fori_loop(0, NQ // GRP, jbody, jnp.zeros((ROWS, NB), F32))
    jp[0] = jacc[:, :128]
    jp[1] = jacc[:, 128:]
    j_copy = pltpu.make_async_remote_copy(
        src_ref=jp.at[1 - y], dst_ref=jr, send_sem=j_s, recv_sem=j_r,
        device_id={'aux': 1 - y}, device_id_type=MESH)
    j_copy.start()
    issue(I5)

    relay(1, 0)

    acc = zero
    for h in range(2):
        issue(6 + 2 * h)
        acc = off_part(0, 1, h * half, half, lt.at[0, h], acc)
    off_done(0, 1, acc)

    def finish_kd(spin):
        total = kd[spin, c]
        for d in range(1, 4):
            s = lax.rem(2 * y + c + d, 4)
            landed(gd.at[spin, s], gd_r.at[spin, s])
            total = total + gd[spin, s]
        s_ref[spin * 64:spin * 64 + 64, :] = total

    def finish_ko(spin):
        pair_sum = []
        for cs in range(2):
            total = kp[spin, cs, c]
            for d in range(1, 4):
                s = lax.rem(2 * y + c + d, 4)
                landed(gp.at[spin, cs, s], gp_r.at[spin, cs, s])
                total = total + gp[spin, cs, s]
            pair_sum.append(total)
        if spin == 0:
            landed(kr.at[0, 1], kr_r.at[0])
            turned = kr[0, 1]
        else:
            @pl.when(c == 0)
            def _():
                landed(kr.at[1, 1], kr_r.at[1])

            @pl.when(c == 1)
            def _():
                for s in range(4):
                    landed(gt.at[s], gt_r.at[s])
                kr[1, 1] = (gt[0] + gt[1]) + (gt[2] + gt[3])
            turned = kr[1, 1]
        a, b = pair_sum
        left = lax.broadcasted_iota(jnp.int32, (32, 128), 1) < 64
        s_ref[spin * 64:spin * 64 + 32, :] = turned[:32] + jnp.where(left, a, pltpu.roll(b, 64, 1))
        s_ref[spin * 64 + 32:spin * 64 + 64, :] = turned[32:] + jnp.where(left, pltpu.roll(a, 64, 1), b)

    acc = zero
    for j, count in ((0, half), (half, 1), (half + 1, 1), (half + 2, 1)):
        issue(10 if j == 0 else 12)
        acc = off_part(1, 1, j, count, lt.at[1, 0] if j == 0 else lc.at[j - half], acc)
        if j == 0:
            issue(12)
            relay(0, 1)
            j_copy.wait()
            jout_ref[...] = jp[y] + jr[...]

            @pl.when(x == y)
            def _():
                finish_kd(0)
                finish_kd(1)

            @pl.when(x != y)
            def _():
                finish_ko(0)
    off_done(1, 1, acc)

    @pl.when(x != y)
    def _():
        finish_ko(1)

    for spin in range(2):
        each_kd(spin, wait_send)
        for cs in range(2):
            each_ko(spin, cs, wait_send)
        for j in range(CHUNKS):
            for k in range(2):
                partner_send(spin, k, j).wait_send()

    @pl.when(c == 0)
    def _():
        for item in items[SWITCH:]:
            remote_send(*item).wait_send()

    @pl.when(c == 1)
    def _():
        for item in turns[-DEPTH:]:
            remote_send(*item).wait_send()

    for spin, cs in ((0, 0), (1, 0), (0, 1)):
        @pl.when(jnp.logical_and(y == hub(spin, cs), c == cs))
        def _():
            kr_send(spin, cs).wait_send()

    for d in range(1, 4):
        gamma_send(d).wait_send()


def solution(mesh):
    def local_build(b_local, c_alpha, c_beta):
        b_rows = b_local.reshape(NQ * ROWS, NB)
        dma = pltpu.SemaphoreType.DMA
        vmem = pltpu.VMEM
        neg, coul = pl.pallas_call(
            kernel,
            out_shape=[pltpu.VMEM((2 * ROWS, 128), F32), pltpu.VMEM((ROWS, 128), F32)],
            in_specs=[pl.BlockSpec(memory_space=pl.ANY)] * 3,
            out_specs=[pl.BlockSpec(memory_space=vmem)] * 2,
            scratch_shapes=[
                vmem((NQ * ROWS, NB), F32),
                vmem((2, 8, TROWS, 128), F32),
                vmem((20, NB), F32), vmem((19, NB), F32),
                vmem((40, NB), F32), vmem((120, NB), BF16), vmem((40, NB), F32),
                vmem((128, NB), F32),
                vmem((4, 8, 128), F32),
                vmem((GRP, 128, 128), F32),
                vmem((2, 2, 384, CHUNKS * CROWS[0]), BF16),
                vmem((CHUNKS // 2, 384, 384), BF16),
                vmem((2, 2, 64, 128), F32), vmem((2, 2, 2, 32, 128), F32), vmem((2, 2, 64, 128), F32),
                vmem((2, 2, 64, 128), F32),
                vmem((2, 4, 64, 128), F32), vmem((2, 2, 4, 32, 128), F32), vmem((4, 64, 128), F32),
                vmem((2, 4, 64, 128), F32),
                vmem((2, 64, 128), F32), vmem((64, 128), F32),
                dma((4, CHUNKS)), dma((2,)),
                dma((2, 2, CHUNKS)), dma((2, 2, CHUNKS)),
                dma((2, 2, CHUNKS)), dma((2, 2, CHUNKS)),
                dma((4,)), dma((4,)),
                dma((2, 2)), dma((2, 4)), dma((2, 2, 2)), dma((2, 2, 4)), dma, dma((4,)),
                dma((2, 2)), dma((2, 4)), dma((2,)), dma((2,)),
                dma, dma, pltpu.SemaphoreType.REGULAR,
            ],
            compiler_params=pltpu.CompilerParams(
                collective_id=0, has_side_effects=True, vmem_limit_bytes=56 * 1024 * 1024),
        )(b_rows, c_alpha.T, c_beta.T)
        return coul - neg[:ROWS], coul - neg[ROWS:]

    spec_b = P(('sys', 'aux'), 'orb', None)
    spec_c = P('sys', None)
    spec_g = P(('sys', 'orb'), 'aux')
    return jax.shard_map(local_build, mesh=mesh, in_specs=(spec_b, spec_c, spec_c), out_specs=(spec_g, spec_g), check_vma=False)
```

```python
import jax
import jax.numpy as jnp
from jax import lax
from jax.experimental import pallas as pl
from jax.experimental.pallas import tpu as pltpu
from jax.sharding import PartitionSpec as P

TOP = lax.Precision.HIGHEST
MESH = pl.DeviceIdType.MESH
F32 = jnp.float32

NQ = 384
ROWS = 64
NB = 256
GRP = 4
QGROUPS = 24
CHUNKS = 6
CGROUPS = QGROUPS // CHUNKS
CROWS = (CGROUPS * 40, CGROUPS * 38)
BCH = CGROUPS * GRP * ROWS
TROWS = CHUNKS * CROWS[0]
SWITCH = 14
LAST = ((1, 3), (0, 3), (1, 4), (1, 5), (0, 4), (0, 5))
IA, I0, I1, I2, IT, I3, I4, I5 = 1, 1, 1, 1, 4, 4, 5, 6
AHEAD = 4
DEPTH = 6
LANES = 128
SIDE = 64
PACK = 32
ORBS = 40
BODY = 16
NT, NN, TN = ((1,), (1,)), ((1,), (0,)), ((0,), (0,))


def dot(a, b, dims):
    return lax.dot_general(a, b, (dims, ((), ())), precision=TOP, preferred_element_type=F32)


BF16 = jnp.bfloat16
SHRINK = 1.0 - 2.0 ** -9


def split(v):
    v1 = (v * SHRINK).astype(BF16)
    rest = v - v1.astype(F32)
    v2 = rest.astype(BF16)
    return v1, v2, (rest - v2.astype(F32)).astype(BF16)


def dot16(a, b, dims):
    return lax.dot_general(a, b, (dims, ((), ())), preferred_element_type=F32)


def kernel(b_hbm, ca_hbm, cb_hbm, s_ref, jout_ref,
           bv, tb, cav, cbv, ct, cs, crep, sacc, gam, grep, lt, lc, kd, kp, kt, kr, gd, gp, gt, gr, jp, jr,
           bsem, csem, rs_s, rs_r, ps_s, ps_r, gm_s, gm_r, gd_s, gd_r, gp_s, gp_r, gt_s, gt_r, gr_s, gr_r, kr_s, kr_r, j_s, j_r, turn):
    o = lax.axis_index('orb')
    y = lax.axis_index('aux')
    x = o // 2
    c = o % 2
    par = 2 * x + (1 - c)
    far = 2 * (1 - x)

    quarter = (far + c, far + (1 - c), par, o)
    slot = (4 + c, 6, 7, c)

    def bcopy(kind, j):
        start = pl.multiple_of((quarter[kind] * CHUNKS + j) * BCH, BCH)
        return pltpu.make_async_copy(b_hbm.at[pl.ds(start, BCH)], bv.at[pl.ds(start, BCH)], bsem.at[kind, j])

    order = [(k, j) for j in range(CHUNKS) for k in (0, 1)] + [(k, j) for k in (2, 3) for j in range(CHUNKS)]
    ca_copy = pltpu.make_async_copy(ca_hbm, cav, csem.at[0])
    cb_copy = pltpu.make_async_copy(cb_hbm, cbv, csem.at[1])
    def bpiece(kind, j, u):
        rows = BCH // 4
        start = pl.multiple_of((quarter[kind] * CHUNKS + j) * BCH + u * rows, rows)
        return pltpu.make_async_copy(b_hbm.at[pl.ds(start, rows)], bv.at[pl.ds(start, rows)], bsem.at[kind, j])

    for u in range(4):
        bpiece(0, 0, u).start()
    ca_copy.start()
    cb_copy.start()
    for k, j in order[1:1]:
        for u in range(4):
            bpiece(k, j, u).start()
    for k, j in order[1:AHEAD]:
        bcopy(k, j).start()

    barrier = pltpu.get_barrier_semaphore()
    def greet(yd, od):
        pl.semaphore_signal(barrier, inc=1, device_id={'aux': yd, 'orb': od}, device_id_type=MESH)

    greet(y, par)
    for od in (far, far + 1):
        greet(y, od)
    for od in (2 * x, 2 * x + 1):
        greet(1 - y, od)

    @pl.when(x != y)
    def _():
        for od in (far, far + 1):
            greet(1 - y, od)

    ca_copy.wait()
    cb_copy.wait()
    ct[0:BODY, :] = cav[0:BODY, :]
    ct[BODY:PACK, :] = cbv[0:BODY, :]
    ct[PACK:36, :] = cav[BODY:20, :]
    ct[36:39, :] = cbv[BODY:19, :]
    ct[39:ORBS, :] = jnp.zeros((1, NB), F32)
    cs[...] = jnp.concatenate([t.astype(F32) for t in split(ct[...])], axis=0).astype(BF16)
    own = ct[:, pl.ds(pl.multiple_of(x * LANES, LANES), LANES)]
    turned = pltpu.roll(own, SIDE, 1)
    low = lax.broadcasted_iota(jnp.int32, (ORBS, LANES), 1) < SIDE
    own = jnp.where(low, jnp.where(c == 0, own, turned), jnp.where(c == 0, turned, own))
    crep[:, :LANES] = own
    crep[:, LANES:] = own
    sacc[96:LANES, :] = jnp.zeros((PACK, NB), F32)

    def part(spin, s, j, count=1):
        return tb.at[spin, s, pl.ds(pl.multiple_of(j * CROWS[spin], 8), count * CROWS[spin])]

    def half_transform(kind, j):
        bcopy(kind, j).wait()
        first = (quarter[kind] * CHUNKS + j) * CGROUPS
        to_a = part(0, slot[kind], j)
        to_b = part(1, slot[kind], j)
        for h in range(CGROUPS // 2):
            base = pl.multiple_of((first + 2 * h) * NB, NB)
            b1, b2, b3 = split(bv[pl.ds(base, 512), :])
            r1 = dot16(cs[...], b1, NT)
            r2 = dot16(cs[0:80, :], b2, NT)
            r3 = dot16(cs[0:ORBS, :], b3, NT)
            r2 = ((r3 + r2[ORBS:80] + r1[80:120]) + (r2[0:ORBS] + r1[ORBS:80])) + r1[0:ORBS]
            for u in range(4):
                p = 4 * h + u
                r = r2[:, u * LANES:(u + 1) * LANES]
                to_a[BODY * p:BODY * p + BODY, :] = r[0:BODY]
                to_b[BODY * p:BODY * p + BODY, :] = r[BODY:PACK]
                to_a[LANES + 4 * p:132 + 4 * p, :] = r[PACK:36]
                to_b[LANES + 3 * p:131 + 3 * p, :] = r[36:39]
            for u in range(2):
                r = r2[:, u * NB:(u + 1) * NB]
                sacc[pl.ds(first + 2 * h + u, 1), :] = jnp.sum(r * crep[...], axis=0, keepdims=True)

    def remote_send(spin, kind, j, count=1):
        return pltpu.make_async_remote_copy(
            src_ref=part(spin, slot[kind], j, count), dst_ref=part(spin, 2 + c, j, count),
            send_sem=rs_s.at[spin, kind, j], recv_sem=rs_r.at[spin, c, j],
            device_id={'orb': quarter[kind]}, device_id_type=MESH)

    def partner_send(spin, which, j):
        return pltpu.make_async_remote_copy(
            src_ref=part(spin, 6 + which, j), dst_ref=part(spin, (4 + c) if which == 0 else c, j),
            send_sem=ps_s.at[spin, which, j], recv_sem=ps_r.at[spin, which, j],
            device_id={'orb': par}, device_id_type=MESH)

    def partner_recv(spin, which, j):
        return pltpu.make_async_remote_copy(
            src_ref=part(spin, 6, j), dst_ref=part(spin, (5 - c) if which == 0 else (1 - c), j),
            send_sem=ps_s.at[spin, which, j], recv_sem=ps_r.at[spin, which, j],
            device_id={'orb': par}, device_id_type=MESH)

    half = CHUNKS // 2
    items = [(0, k, j, 1) for k, j in order[:2 * CHUNKS]] + [(1, k, j, half) for j in (0, half) for k in (0, 1)]
    turns = [(0, k, j, half) for j in (0, half) for k in (1, 0)] + [(1, k, 0, half) for k in (1, 0)]
    turns += [(1, k, j, 1) for k, j in LAST]
    issued = [0]
    issued = [0]

    def issue(upto):
        todo = range(issued[0], min(upto, len(turns)))
        issued[0] = max(issued[0], min(upto, len(turns)))

        @pl.when(c == 1)
        def _():
            for n in todo:
                if n >= DEPTH:
                    remote_send(*turns[n - DEPTH]).wait_send()
                remote_send(*turns[n]).start()

    half_transform(0, 0)
    for k, j in order[AHEAD:]:
        bcopy(k, j).start()
    pl.semaphore_wait(barrier, jnp.where(x == y, 5, 7))

    @pl.when(c == 0)
    def _():
        remote_send(0, 0, 0).start()

    half_transform(1, 0)

    @pl.when(c == 0)
    def _():
        remote_send(0, 1, 0).start()

    def pair(j, _):
        for k in (0, 1):
            half_transform(k, j)

            @pl.when(c == 0)
            def _():
                remote_send(0, k, j).start()
        for spin in range(2):
            partner_send(spin, 0, j).start()
        return 0

    for spin in range(2):
        partner_send(spin, 0, 0).start()
    lax.fori_loop(1, CHUNKS, pair, 0)
    issue(IA)

    def back(j, _):
        half_transform(2, j)
        for spin in range(2):
            partner_send(spin, 1, j).start()
        return 0

    lax.fori_loop(0, CHUNKS, back, 0)

    @pl.when(c == 0)
    def _():
        for item in items[2 * CHUNKS:]:
            remote_send(*item).start()

    def home(j, _):
        half_transform(3, j)
        return 0

    lax.fori_loop(0, CHUNKS, home, 0)
    issue(I0)

    e8 = (lax.broadcasted_iota(jnp.int32, (8, NB), 1) // ROWS == lax.broadcasted_iota(jnp.int32, (8, NB), 0)).astype(F32)
    gam[o] = dot(e8, sacc[...], NT)

    def gamma_send(d):
        return pltpu.make_async_remote_copy(
            src_ref=gam.at[o], dst_ref=gam.at[o], send_sem=gm_s.at[d], recv_sem=gm_r.at[d],
            device_id={'orb': lax.rem(o + d, 4)}, device_id_type=MESH)

    def gamma_recv(d):
        src = lax.rem(o + 4 - d, 4)
        return pltpu.make_async_remote_copy(
            src_ref=gam.at[src], dst_ref=gam.at[src], send_sem=gm_s.at[d], recv_sem=gm_r.at[d],
            device_id={'orb': par}, device_id_type=MESH)

    for d in range(1, 4):
        gamma_send(d).start()

    def sides(spin, s, j, count):
        rows = count * CROWS[spin]
        at = pl.ds(pl.multiple_of(j * CROWS[spin], 8), rows)
        a = tb[spin, s, at]
        b = tb[spin, s + 1, at]
        left = lax.broadcasted_iota(jnp.int32, (rows, LANES), 1) < SIDE
        return jnp.where(left, a, pltpu.roll(b, SIDE, 1)), jnp.where(left, pltpu.roll(a, SIDE, 1), b)

    for spin in range(2):
        cols = 2 * half * CROWS[spin]
        acc = (jnp.zeros((LANES, LANES), F32),) * 2
        for which in range(2):
            def dbody(h, acc):
                for u in range(half):
                    partner_recv(spin, which, h * half + u).wait_recv()
                m = jnp.concatenate(sides(spin, (4, 0)[which], h * half, half), axis=0)
                m1, m2, m3 = split(m)
                t1, t2, t3 = split(m.T)
                r = dot16(jnp.concatenate([t1, t2], axis=0), jnp.concatenate([m1, m2], axis=1), NN)
                q = dot16(t1, m3, NN)
                if which == 1:
                    lt[spin, h, :, 0:cols] = jnp.concatenate([t1, t2, t3], axis=0)
                return acc[0] + ((r[LANES:, LANES:] + (r[:LANES, LANES:] + r[LANES:, :LANES])) + r[:LANES, :LANES]), acc[1] + q
            acc = lax.fori_loop(0, 2, dbody, acc)
        acc = acc[0] + (acc[1] + acc[1].T)
        kd[spin, 0] = acc[:SIDE]
        kd[spin, 1] = acc[SIDE:]
        if spin == 1:
            for u in range(half):
                lc[u, :, 0:2 * CROWS[1]] = jnp.concatenate(split(jnp.concatenate(sides(1, 0, half + u, 1), axis=0).T), axis=0)
        issue(I1 if spin == 0 else I2)

    def kd_send(spin, cd):
        return pltpu.make_async_remote_copy(
            src_ref=kd.at[spin, cd], dst_ref=gd.at[spin, 2 * y + c],
            send_sem=gd_s.at[spin, cd], recv_sem=gd_r.at[spin, 2 * y + c],
            device_id={'aux': x, 'orb': 2 * x + cd}, device_id_type=MESH)

    def kp_send(spin, cs, cd):
        return pltpu.make_async_remote_copy(
            src_ref=kp.at[spin, cs, cd], dst_ref=gp.at[spin, cs, 2 * y + c],
            send_sem=gp_s.at[spin, cs, cd], recv_sem=gp_r.at[spin, cs, 2 * y + c],
            device_id={'aux': 1 - x, 'orb': 2 * x + cd}, device_id_type=MESH)

    def kt_send(spin):
        return pltpu.make_async_remote_copy(
            src_ref=kt.at[spin, 1], dst_ref=gt.at[2 * y + c],
            send_sem=gt_s, recv_sem=gt_r.at[2 * y + c],
            device_id={'aux': x, 'orb': 2 * (1 - x) + 1}, device_id_type=MESH)

    def hub(spin, cs):
        return x if (spin, cs) in ((0, 0), (1, 0)) else 0

    def gr_send(spin, cs):
        return pltpu.make_async_remote_copy(
            src_ref=kt.at[spin, cs], dst_ref=gr.at[spin, 2 * y + c],
            send_sem=gr_s.at[spin, cs], recv_sem=gr_r.at[spin, 2 * y + c],
            device_id={'aux': hub(spin, cs), 'orb': 2 * x + cs}, device_id_type=MESH)

    def kr_send(spin, cs):
        return pltpu.make_async_remote_copy(
            src_ref=kr.at[spin, 0], dst_ref=kr.at[spin, 1],
            send_sem=kr_s.at[spin], recv_sem=kr_r.at[spin],
            device_id={'aux': x, 'orb': 2 * (1 - x) + cs}, device_id_type=MESH)

    def relay(spin, cs):
        @pl.when(jnp.logical_and(y == hub(spin, cs), c == cs))
        def _():
            total = kt[spin, cs]
            for d in range(1, 4):
                s = lax.rem(2 * y + c + d, 4)
                landed(gr.at[spin, s], gr_r.at[spin, s])
                total = total + gr[spin, s]
            kr[spin, 0] = total
            kr_send(spin, cs).start()

    def landed(dst, sem):
        return pltpu.make_async_remote_copy(
            src_ref=dst, dst_ref=dst, send_sem=j_s, recv_sem=sem, device_id={'orb': par}, device_id_type=MESH).wait_recv()

    start = lambda copy: copy.start()
    wait_send = lambda copy: copy.wait_send()

    def each_kd(spin, act):
        for cd in range(2):
            @pl.when(jnp.logical_not(jnp.logical_and(x == y, c == cd)))
            def _():
                act(kd_send(spin, cd))

    def each_ko(spin, cs, act):
        if (spin, cs) == (1, 1):
            act(kt_send(spin))
        else:
            @pl.when(jnp.logical_not(jnp.logical_and(y == hub(spin, cs), c == cs)))
            def _():
                act(gr_send(spin, cs))
        for cd in range(2):
            @pl.when(jnp.logical_not(jnp.logical_and(x != y, c == cd)))
            def _():
                act(kp_send(spin, cs, cd))

    for spin in range(2):
        each_kd(spin, start)

    @pl.when(c == 0)
    def _():
        for item in items[:SWITCH]:
            remote_send(*item).wait_send()
        pl.semaphore_signal(turn, inc=1, device_id={'orb': par}, device_id_type=MESH)

    @pl.when(c == 1)
    def _():
        pl.semaphore_wait(turn, 1)

    issue(IT)

    def off_part(spin, cs, j, count, left_side, acc):
        step = 1 if (spin, cs) == (0, 0) else count
        for u in range(0, count, step):
            landed(part(spin, 2 + cs, j + u, step), rs_r.at[spin, cs, j + u])
        rows = count * CROWS[spin]
        v = tb[spin, 2 + cs, j * CROWS[spin]:j * CROWS[spin] + rows]
        v1, v2, v3 = [t.astype(F32) for t in split(v)]
        left = lax.broadcasted_iota(jnp.int32, (rows, LANES), 1) < SIDE
        none = jnp.zeros((rows, LANES), F32)
        w = jnp.concatenate([
            jnp.concatenate([jnp.where(left, v1, pltpu.roll(v2, SIDE, 1)), jnp.where(left, v3, none)], axis=1),
            jnp.concatenate([jnp.where(left, pltpu.roll(v1, SIDE, 1), v2), jnp.where(left, pltpu.roll(v3, SIDE, 1), none)], axis=1),
        ], axis=0).astype(BF16)
        r = dot16(left_side[:, 0:2 * rows], w, NN)
        return acc + ((r[NB:] + r[LANES:NB]) + r[:LANES])

    def off_done(spin, cs, acc):
        block = acc[:, :LANES] + acc[:, LANES:]
        block = block + pltpu.roll(block, SIDE, 1)
        left = lax.broadcasted_iota(jnp.int32, (PACK, LANES), 1) < SIDE
        kt[spin, cs] = block.T[:SIDE]
        for cd in range(2):
            kp[spin, cs, cd] = jnp.where(left, block[SIDE * cd:SIDE * cd + PACK], pltpu.roll(block[SIDE * cd + PACK:SIDE * cd + SIDE], SIDE, 1))
        each_ko(spin, cs, start)

    zero = jnp.zeros((LANES, NB), F32)
    for spin in range(2):
        acc = zero
        for h in range(2):
            acc = off_part(spin, 0, h * half, half, lt.at[spin, h], acc)
        off_done(spin, 0, acc)
        issue(I3 if spin == 0 else I4)
        if spin == 1:
            relay(0, 0)

    for d in range(1, 4):
        gamma_recv(d).wait_recv()
    gsum = (gam[0] + gam[1]) + (gam[2] + gam[3])
    for k in range(GRP):
        pick = (lax.broadcasted_iota(jnp.int32, (8, LANES), 0) == k).astype(F32)
        grep[k] = dot(gsum, pick, TN)

    def jbody(g, acc):
        for k in range(GRP):
            row = grep[k, pl.ds(g, 1), :]
            base = pl.multiple_of(g * NB + k * ROWS, ROWS)
            acc = acc + bv[pl.ds(base, ROWS), :] * jnp.concatenate([row, row], axis=1)
        return acc

    jacc = lax.fori_loop(0, NQ // GRP, jbody, jnp.zeros((ROWS, NB), F32))
    jp[0] = jacc[:, :LANES]
    jp[1] = jacc[:, LANES:]
    j_copy = pltpu.make_async_remote_copy(
        src_ref=jp.at[1 - y], dst_ref=jr, send_sem=j_s, recv_sem=j_r,
        device_id={'aux': 1 - y}, device_id_type=MESH)
    j_copy.start()
    issue(I5)

    relay(1, 0)

    acc = zero
    for h in range(2):
        issue(6 + 2 * h)
        acc = off_part(0, 1, h * half, half, lt.at[0, h], acc)
    off_done(0, 1, acc)

    def finish_kd(spin):
        total = kd[spin, c]
        for d in range(1, 4):
            s = lax.rem(2 * y + c + d, 4)
            landed(gd.at[spin, s], gd_r.at[spin, s])
            total = total + gd[spin, s]
        s_ref[spin * SIDE:spin * SIDE + SIDE, :] = total

    def finish_ko(spin):
        pair_sum = []
        for cs in range(2):
            total = kp[spin, cs, c]
            for d in range(1, 4):
                s = lax.rem(2 * y + c + d, 4)
                landed(gp.at[spin, cs, s], gp_r.at[spin, cs, s])
                total = total + gp[spin, cs, s]
            pair_sum.append(total)
        if spin == 0:
            landed(kr.at[0, 1], kr_r.at[0])
            turned = kr[0, 1]
        else:
            @pl.when(c == 0)
            def _():
                landed(kr.at[1, 1], kr_r.at[1])

            @pl.when(c == 1)
            def _():
                for s in range(4):
                    landed(gt.at[s], gt_r.at[s])
                kr[1, 1] = (gt[0] + gt[1]) + (gt[2] + gt[3])
            turned = kr[1, 1]
        a, b = pair_sum
        left = lax.broadcasted_iota(jnp.int32, (PACK, LANES), 1) < SIDE
        s_ref[spin * SIDE:spin * SIDE + PACK, :] = turned[:PACK] + jnp.where(left, a, pltpu.roll(b, SIDE, 1))
        s_ref[spin * SIDE + PACK:spin * SIDE + SIDE, :] = turned[PACK:] + jnp.where(left, pltpu.roll(a, SIDE, 1), b)

    acc = zero
    for j, count in ((0, half), (half, 1), (half + 1, 1), (half + 2, 1)):
        issue(10 if j == 0 else 12)
        acc = off_part(1, 1, j, count, lt.at[1, 0] if j == 0 else lc.at[j - half], acc)
        if j == 0:
            issue(12)
            relay(0, 1)
            j_copy.wait()
            jout_ref[...] = jp[y] + jr[...]

            @pl.when(x == y)
            def _():
                finish_kd(0)
                finish_kd(1)

            @pl.when(x != y)
            def _():
                finish_ko(0)
    off_done(1, 1, acc)

    @pl.when(x != y)
    def _():
        finish_ko(1)

    for spin in range(2):
        each_kd(spin, wait_send)
        for cs in range(2):
            each_ko(spin, cs, wait_send)
        for j in range(CHUNKS):
            for k in range(2):
                partner_send(spin, k, j).wait_send()

    @pl.when(c == 0)
    def _():
        for item in items[SWITCH:]:
            remote_send(*item).wait_send()

    @pl.when(c == 1)
    def _():
        for item in turns[-DEPTH:]:
            remote_send(*item).wait_send()

    for spin, cs in ((0, 0), (1, 0), (0, 1)):
        @pl.when(jnp.logical_and(y == hub(spin, cs), c == cs))
        def _():
            kr_send(spin, cs).wait_send()

    for d in range(1, 4):
        gamma_send(d).wait_send()


def solution(mesh):
    def local_build(b_local, c_alpha, c_beta):
        b_rows = b_local.reshape(NQ * ROWS, NB)
        dma = pltpu.SemaphoreType.DMA
        vmem = pltpu.VMEM
        neg, coul = pl.pallas_call(
            kernel,
            out_shape=[pltpu.VMEM((2 * ROWS, LANES), F32), pltpu.VMEM((ROWS, LANES), F32)],
            in_specs=[pl.BlockSpec(memory_space=pl.ANY)] * 3,
            out_specs=[pl.BlockSpec(memory_space=vmem)] * 2,
            scratch_shapes=[
                vmem((NQ * ROWS, NB), F32),
                vmem((2, 8, TROWS, LANES), F32),
                vmem((20, NB), F32), vmem((19, NB), F32),
                vmem((ORBS, NB), F32), vmem((120, NB), BF16), vmem((ORBS, NB), F32),
                vmem((LANES, NB), F32),
                vmem((4, 8, LANES), F32),
                vmem((GRP, LANES, LANES), F32),
                vmem((2, 2, 384, CHUNKS * CROWS[0]), BF16),
                vmem((CHUNKS // 2, 384, 384), BF16),
                vmem((2, 2, SIDE, LANES), F32), vmem((2, 2, 2, PACK, LANES), F32), vmem((2, 2, SIDE, LANES), F32),
                vmem((2, 2, SIDE, LANES), F32),
                vmem((2, 4, SIDE, LANES), F32), vmem((2, 2, 4, PACK, LANES), F32), vmem((4, SIDE, LANES), F32),
                vmem((2, 4, SIDE, LANES), F32),
                vmem((2, SIDE, LANES), F32), vmem((SIDE, LANES), F32),
                dma((4, CHUNKS)), dma((2,)),
                dma((2, 2, CHUNKS)), dma((2, 2, CHUNKS)),
                dma((2, 2, CHUNKS)), dma((2, 2, CHUNKS)),
                dma((4,)), dma((4,)),
                dma((2, 2)), dma((2, 4)), dma((2, 2, 2)), dma((2, 2, 4)), dma, dma((4,)),
                dma((2, 2)), dma((2, 4)), dma((2,)), dma((2,)),
                dma, dma, pltpu.SemaphoreType.REGULAR,
            ],
            compiler_params=pltpu.CompilerParams(
                collective_id=0, has_side_effects=True, vmem_limit_bytes=56 * 1024 * 1024),
        )(b_rows, c_alpha.T, c_beta.T)
        return coul - neg[:ROWS], coul - neg[ROWS:]

    spec_b = P(('sys', 'aux'), 'orb', None)
    spec_c = P('sys', None)
    spec_g = P(('sys', 'orb'), 'aux')
    return jax.shard_map(local_build, mesh=mesh, in_specs=(spec_b, spec_c, spec_c), out_specs=(spec_g, spec_g), check_vma=False)
```
